512 devices in a mesh: pert: 2 (over y), ga: 32 (over z), band: 8 (over x, core).
Axes of the slice: x: 4, y: 2, z: 32, core: 2. Of those that a mesh axis runs over, the one named last changes fastest.
The devices are a block of a 4x8x32 slice.
Arguments:
- psi: float32 [2, 8, 131072], P(None, 'band', 'ga'), may hold values from -6 to 6
- potential: float32 [256, 128, 128], P('pert', 'ga'), parts along dimension 0, may hold values from 1 to 3
- miller: int32 [131072], replicated, may hold values from 0 to 2097151, as said below
- occupied: int32 [8], replicated, may hold values 0 or 1
Outputs:
- projected: float32 [2, 16, 131072], P(None, ('pert', 'band'), 'ga'), parts along dimension 1
The draws below stay inside these ranges and needn't reach their ends.
There are 2 independent parts, one for each index of `pert`. The reference program is written for one: setup_inputs(seed, part) draws one part's arguments, and reference() takes and returns one part's arrays. A program takes and returns all parts, laid end to end along the dimension named above; an argument that names none is the same for every part. Nothing has to cross between parts.
Inputs may be any that keep to these rules, and one draw needn't show every extreme that they name: `miller`: entry k is the flat index a 128^2 + b * 128 + c of coefficient k, with Fourier indices a, b, c in 0..127 taken modulo 128; the entries are distinct; each of a, b, c, read as a signed index in -64..128/2-1, lies in -32..128/4-1; the j-th block of 4096 entries holds only points whose signed a plus 128/4 is congruent to j modulo 131072/4096.
All inputs are finite; a program needn't handle non-finite values.
Results may differ from the reference program's by a relative error of at most 0.00013.
Values sent between devices are 32-bit elements; how exact they have to be, the bound alone decides.
No kernel may reach another device: no remote copies, remote signals or barrier semaphores. Data moves between devices by JAX's collectives and lax.ppermute only.
A program may use at most 64 MiB of HBM per device.

```python
import jax
import jax.numpy as jnp
from jax import lax

N = 128
NPW = 131072
NB = 8
PW_SHARD = 4096


def draw_miller(key, part):
    owners = NPW // PW_SHARD
    quarter = N // 4
    per_owner = N * N * N // owners
    slot_index = jnp.arange(per_owner, dtype=jnp.int32)
    owner_index = jnp.arange(owners, dtype=jnp.int32)[:, None]
    plane_index = slot_index // (N * N)
    remainder = slot_index % (N * N)
    row_index = remainder // N
    column_index = remainder % N
    plane_pos = owner_index + owners * plane_index
    signed_a = plane_pos - quarter
    signed_b = row_index - quarter
    signed_c = column_index - quarter
    inside = (plane_pos < N // 2) & (row_index < N // 2)[None, :] & (column_index < N // 2)[None, :]
    radius = signed_a * signed_a + (signed_b * signed_b + signed_c * signed_c)[None, :]
    limit = 2 ** 31 // per_owner - 1
    keys = jax.random.split(key, owners)
    breaker = jax.vmap(lambda sub_key: jax.random.permutation(sub_key, per_owner))(keys).astype(jnp.int32)
    score = jnp.where(inside, jnp.minimum(radius, limit - 1), limit) * per_owner + breaker
    order = jnp.argsort(score, axis=1)[:, :PW_SHARD]
    unsigned_a = (plane_pos + N - quarter) % N
    unsigned_b = (row_index + N - quarter) % N
    unsigned_c = (column_index + N - quarter) % N
    flat_index = unsigned_a * (N * N) + (unsigned_b * N + unsigned_c)[None, :]
    return jnp.take_along_axis(flat_index, order, axis=1).reshape(NPW).astype(jnp.int32)


def plant(values, stream_key, low, largest):
    index_at = [jax.random.randint(jax.random.fold_in(stream_key, axis), (), 0, length) for axis, length in enumerate(values.shape)]
    longest = values.shape.index(max(values.shape))
    neighbour = index_at[:longest] + [(index_at[longest] + 1) % values.shape[longest]] + index_at[longest + 1:]
    return values.at[tuple(index_at)].set(low).at[tuple(neighbour)].set(largest)


def levels(key, extent, cuts, low, high):
    def one(axis_at, parts):
        steps = jax.random.uniform(jax.random.fold_in(jax.random.fold_in(key, 6), axis_at), (parts,), jnp.float32, low / len(cuts), high / len(cuts))
        return jnp.repeat(jnp.exp(steps), extent[axis_at] // parts).reshape((-1,) + (1,) * (len(extent) - axis_at - 1))

    factor_of = one(*cuts[0])
    for cut in cuts[1:]:
        factor_of = factor_of * one(*cut)
    return factor_of


def noise(own_key, extent, scale, most, cuts=(), kind=jnp.bfloat16):
    gain = levels(own_key, extent, cuts, -0.22, 0.18) if cuts else 1.0
    entries = jax.random.normal(own_key, extent, jnp.float32) * scale * gain
    return jnp.minimum(jnp.maximum(entries, -most), most).astype(kind)


def setup_inputs(seed: int = 0, part: int = 0) -> dict:
    arg_keys = jax.random.split(jax.random.key(seed), 5)
    part_splits = jax.random.split(jax.random.fold_in(arg_keys[4], part), 5)
    psi = noise(arg_keys[0], (2, NB, NPW), 1.0, 6.0, ((1, 8), (2, 32)), jnp.float32)
    potential = jnp.clip(1.0 + 2.0 * jax.random.uniform(part_splits[1], (N, N, N), jnp.float32) ** levels(part_splits[1], (N, N, N), ((1, 32),), -0.2, 0.2), 1.0, 3.0)
    miller = draw_miller(jax.random.fold_in(arg_keys[4], 71), part)
    occupied = plant((jax.random.randint(arg_keys[3], (NB,), 0, 4) < 3).astype(jnp.int32), jax.random.fold_in(arg_keys[3], 1), 0, 1)
    return {"psi": psi, "potential": potential, "miller": miller, "occupied": occupied}


highest = lax.Precision.HIGHEST


def reference(psi, potential, miller, occupied):
    volume = N * N * N

    def apply_one(coefs):
        real_grid = jnp.zeros((volume,), coefs.dtype).at[miller].set(coefs[0])
        imag_grid = jnp.zeros((volume,), coefs.dtype).at[miller].set(coefs[1])
        field_grid = lax.complex(real_grid, imag_grid).reshape(N, N, N)
        wave_grid = jnp.fft.ifftn(field_grid) * volume
        product = wave_grid * potential
        back_grid = (jnp.fft.fftn(product) / volume).reshape(volume)[miller]
        return jnp.stack([jnp.real(back_grid), jnp.imag(back_grid)])

    applied = lax.map(apply_one, jnp.transpose(psi, (1, 0, 2)))
    applied_real = applied[:, 0]
    applied_imag = applied[:, 1]
    basis_real = psi[0]
    basis_imag = psi[1]
    over_real = jnp.dot(basis_real, applied_real.T, precision=highest) + jnp.dot(basis_imag, applied_imag.T, precision=highest)
    over_imag = jnp.dot(basis_real, applied_imag.T, precision=highest) - jnp.dot(basis_imag, applied_real.T, precision=highest)
    weights = occupied.astype(psi.dtype)[:, None]
    weight_real = weights * (over_real / NPW)
    weight_imag = weights * (over_imag / NPW)
    proj_real = jnp.dot(weight_real.T, basis_real, precision=highest) - jnp.dot(weight_imag.T, basis_imag, precision=highest)
    proj_imag = jnp.dot(weight_imag.T, basis_real, precision=highest) + jnp.dot(weight_real.T, basis_imag, precision=highest)
    return jnp.stack([applied_real - proj_real, applied_imag - proj_imag])
```

```python
import functools

import jax
import jax.numpy as jnp
import numpy as np
from jax import lax
from jax.experimental import pallas as pl
from jax.experimental.pallas import tpu as pltpu
from jax.sharding import PartitionSpec as P

highest = lax.Precision.HIGHEST
INTERPRET = False


def dot(a, b):
    return jnp.dot(a, b, precision=highest, preferred_element_type=jnp.float32)


def thirds(x):
    high = x.astype(jnp.bfloat16)
    rest = x - high.astype(jnp.float32)
    mid = rest.astype(jnp.bfloat16)
    low = (rest - mid.astype(jnp.float32)).astype(jnp.bfloat16)
    return high, mid, low


def turned(x):
    half = x.shape[1] // 2
    return jnp.concatenate([-x[:, half:], x[:, :half]], axis=1)


def tables(size, owners):
    kept, per = size // 2, size // (2 * owners)
    signed = np.arange(kept) - size // 4
    full = np.arange(size)
    angle = 2.0 * np.pi / size * (full[:, None] * signed[None, :] % size)
    cosine, sine = np.cos(angle), np.sin(angle)
    rows = [np.einsum("yb,tu->ytub", part, np.eye(per)).reshape(size * per, per * kept) for part in (cosine, sine)]
    along_y = np.concatenate(rows, axis=1)
    along_z = np.block([[cosine.T, sine.T], [-sine.T, cosine.T]])
    along_x = np.block([[cosine, -sine], [sine, cosine]])
    own = size // owners
    back = [part.reshape(owners, own * per, per * kept).transpose(2, 1, 0).reshape(per * kept, size * per) for part in rows]
    back_y = np.concatenate([back[0], -back[1]], axis=1)
    as32 = lambda x: np.asarray(x, np.float32)
    return as32(along_y), as32(along_z), as32(along_x), as32(along_x.T), as32(along_z.T / size**3), as32(back_y)


def places(points, size, owners):
    quarter = size // 4
    plane = (points // (size * size) + quarter) % size
    row = (points // size + quarter) % size
    column = (points + quarter) % size
    return plane // owners * (size // 2) + row, column


def picks(index, count):
    return lax.broadcasted_iota(jnp.int32, (count, index.shape[1]), 0) == index


def spread_kernel(owner_ref, psi_ref, points_ref, along_ref, out_ref, *, size, owners):
    del owner_ref
    line, column = places(points_ref[0], size, owners)
    lines = along_ref.shape[1] // 2
    at_line = picks(line, lines).astype(jnp.bfloat16)
    at_column = picks(column, size // 2)
    zero = jnp.zeros((), jnp.bfloat16)
    total = None
    for real, imag in zip(thirds(psi_ref[0]), thirds(psi_ref[1])):
        spread = jnp.concatenate([jnp.where(at_column, real, zero), jnp.where(at_column, imag, zero)], axis=0)
        term = lax.dot_general(at_line, spread, (((1,), (1,)), ((), ())), preferred_element_type=jnp.float32)
        total = term if total is None else total + term
    out_ref[...] = dot(along_ref[...], jnp.concatenate([total, turned(total)], axis=0))


def apply_kernel(field_ref, potential_ref, z_ref, x_ref, back_x_ref, back_z_ref, out_ref, wide_ref, *, size, owners):
    per, own = size // (2 * owners), size // owners
    group = per * own
    wide = dot(field_ref[...], z_ref[...])
    for part in range(2):
        wide_ref[part] = wide[:, part * size : (part + 1) * size]

    def planes(y, part):
        return [wide_ref[part, pl.ds(y * per + t, owners, stride=group), :] for t in range(per)]

    columns = [jnp.concatenate(planes(y, 0) + planes(y, 1), axis=0) for y in range(own)]
    wave = dot(x_ref[...], jnp.concatenate(columns, axis=1))
    scale = jnp.concatenate([potential_ref[:, y, :] for y in range(own)], axis=1)
    product = jnp.concatenate([wave[:size] * scale, wave[size:] * scale], axis=0)
    back = dot(back_x_ref[...], product)
    for y in range(own):
        for t in range(per):
            for part in range(2):
                first = (part * per + t) * owners
                wide_ref[part, pl.ds(y * per + t, owners, stride=group), :] = back[first : first + owners, y * size : (y + 1) * size]
    out_ref[...] = dot(wide_ref[0], back_z_ref[:size]) + dot(wide_ref[1], back_z_ref[size:])


def pair_kernel(fields_ref, product_ref, out_ref, *, owners):
    bands = fields_ref.shape[0]
    lanes = product_ref.shape[1]
    group = product_ref.shape[0] // owners
    product = product_ref[...]
    half = lanes // 2
    crossed = jnp.concatenate([product[:, half:], -product[:, :half]], axis=1)
    sums = []
    for other in (product, crossed):
        for m in range(bands):
            sums.append(jnp.sum(fields_ref[m].reshape(product.shape) * other, axis=0, keepdims=True))
    sums = jnp.concatenate(sums, axis=0)
    sums = dot(sums, jnp.ones((lanes, lanes), jnp.float32))
    on_diagonal = lax.broadcasted_iota(jnp.int32, sums.shape, 0) == lax.broadcasted_iota(jnp.int32, sums.shape, 1)
    row = jnp.sum(jnp.where(on_diagonal, sums, 0.0), axis=0, keepdims=True)
    for r in range(group):
        out_ref[pl.ds(r, owners, stride=group + 1), :] = product_ref[pl.ds(r, owners, stride=group), :]
    out_ref[pl.ds(group, owners, stride=group + 1), :] = jnp.broadcast_to(row, (owners, lanes))


def project_kernel(owner_ref, occupied_ref, rows_ref, basis_ref, points_ref, along_ref, out_ref, *, size, owners, coefs):
    del owner_ref
    bands = occupied_ref.shape[0]
    group = rows_ref.shape[0] // owners
    sums = jnp.sum(rows_ref[pl.ds(group - 1, owners, stride=group), :], axis=0, keepdims=True)
    rows = jnp.concatenate([rows_ref[pl.ds(r, owners, stride=group), :] for r in range(group - 1)], axis=0)
    lines = dot(along_ref[...], jnp.concatenate([rows, turned(rows)], axis=0))
    line, column = places(points_ref[0], size, owners)
    at_line = picks(line, lines.shape[0]).astype(jnp.bfloat16)
    at_column = picks(column, size // 2)
    found = None
    for part in thirds(lines.T):
        term = jnp.dot(part, at_line, preferred_element_type=jnp.float32)
        found = term if found is None else found + term
    half = size // 2
    applied = [jnp.sum(jnp.where(at_column, found[p * half : (p + 1) * half], 0.0), axis=0, keepdims=True) for p in range(2)]
    tall, lanes = out_ref.shape[1:]
    taken = [jnp.zeros((tall, lanes), jnp.float32) for _ in range(2)]
    for m in range(bands):
        share = occupied_ref[m].astype(jnp.float32)
        weight_real = sums[:, m : m + 1] * (1.0 / coefs) * share
        weight_imag = sums[:, bands + m : bands + m + 1] * (1.0 / coefs) * share
        basis = basis_ref[m].reshape(2, tall, lanes)
        taken[0] = taken[0] + weight_real * basis[0] - weight_imag * basis[1]
        taken[1] = taken[1] + weight_imag * basis[0] + weight_real * basis[1]
    for p in range(2):
        for r in range(tall):
            out_ref[p, r : r + 1, :] = applied[p][:, r * lanes : (r + 1) * lanes] - taken[p][r : r + 1]


def whole(shape):
    return pl.BlockSpec(shape, lambda *_: (0,) * len(shape))


def spread(owner, psi, points, table, size, owners):
    block = points.shape[2]
    return pl.pallas_call(
        functools.partial(spread_kernel, size=size, owners=owners),
        out_shape=jax.ShapeDtypeStruct((table.shape[0], size), jnp.float32),
        grid_spec=pltpu.PrefetchScalarGridSpec(
            num_scalar_prefetch=1,
            grid=(1,),
            in_specs=[whole(psi.shape), pl.BlockSpec((1, 1, block), lambda i, at: (at[0], 0, 0)), whole(table.shape)],
            out_specs=whole((table.shape[0], size)),
        ),
        interpret=INTERPRET,
        name="spread",
    )(owner, psi, points, table)


def apply(field, potential, along_z, along_x, back_x, back_z, size, owners):
    return pl.pallas_call(
        functools.partial(apply_kernel, size=size, owners=owners),
        out_shape=jax.ShapeDtypeStruct(field.shape, jnp.float32),
        scratch_shapes=[pltpu.VMEM((2, *field.shape), jnp.float32)],
        interpret=INTERPRET,
        name="apply",
    )(field, potential, along_z, along_x, back_x, back_z)


def pair(gathered, product, owners):
    bands, tall = gathered.shape[0], product.shape[0] // gathered.shape[2]
    return pl.pallas_call(
        functools.partial(pair_kernel, owners=owners),
        out_shape=jax.ShapeDtypeStruct((product.shape[0] + owners, product.shape[1]), jnp.float32),
        grid=(1,),
        in_specs=[whole((bands, tall, *gathered.shape[2:])), whole(product.shape)],
        out_specs=whole((product.shape[0] + owners, product.shape[1])),
        interpret=INTERPRET,
        name="pair",
    )(gathered, product)


def project(owner, occupied, rows, gathered, points, table, size, owners, block, coefs):
    bands = gathered.shape[0]
    lanes = gathered.shape[3]
    tall = 2 * block // (gathered.shape[2] * lanes)
    last = gathered.shape[1] // tall - 1
    out_shape = (2, block // lanes, lanes)
    return pl.pallas_call(
        functools.partial(project_kernel, size=size, owners=owners, coefs=coefs),
        out_shape=jax.ShapeDtypeStruct(out_shape, jnp.float32),
        grid_spec=pltpu.PrefetchScalarGridSpec(
            num_scalar_prefetch=2,
            grid=(1,),
            in_specs=[
                whole(rows.shape),
                pl.BlockSpec((bands, tall, *gathered.shape[2:]), lambda i, at, occ: (0, last, 0, 0)),
                pl.BlockSpec((1, 1, block), lambda i, at, occ: (at[0], 0, 0)),
                whole(table.shape),
            ],
            out_specs=whole(out_shape),
        ),
        interpret=INTERPRET,
        name="project",
    )(owner, occupied, rows, gathered, points, table)


def shards(psi, potential, miller, occupied):
    size = potential.shape[0]
    owners = lax.axis_size("ga")
    bands = lax.axis_size("band")
    block = psi.shape[2]
    along_y, along_z, along_x, back_x, back_z, back_y = tables(size, owners)
    owner = lax.axis_index("ga").reshape(1)
    points = miller.reshape(-1, 1, block)
    rows = spread(owner, psi, points, along_y, size, owners)
    group = rows.shape[0] // owners
    rows = lax.all_to_all(rows.reshape(owners, group, size), "ga", split_axis=0, concat_axis=0, tiled=True)
    sent = jnp.concatenate([rows, psi.reshape(-1, group, size)], axis=0)
    gathered = lax.all_to_all(jnp.broadcast_to(sent, (bands, *sent.shape)), "band", split_axis=0, concat_axis=0, tiled=True)
    product = apply(rows.reshape(-1, size), potential, along_z, along_x, back_x, back_z, size, owners)
    rows = pair(gathered, product, owners)
    rows = lax.all_to_all(rows.reshape(owners, 1, -1), "ga", split_axis=0, concat_axis=0, tiled=True).reshape(rows.shape)
    out = project(owner, occupied, rows, gathered, points, back_y, size, owners, block, miller.shape[0])
    return out.reshape(2, 1, block)


def solution(mesh):
    in_specs = (P(None, "band", "ga"), P("pert", "ga", None), P(), P())
    out_specs = P(None, ("pert", "band"), "ga")
    return jax.shard_map(shards, mesh=mesh, in_specs=in_specs, out_specs=out_specs, check_vma=False)
```

```python
import functools

import jax
import jax.numpy as jnp
import numpy as np
from jax import lax
from jax.experimental import pallas as pl
from jax.experimental.pallas import tpu as pltpu
from jax.sharding import Mesh
from jax.sharding import PartitionSpec as P

highest = lax.Precision.HIGHEST
INTERPRET = False


def near(x):
    return x if INTERPRET else pltpu.with_memory_space_constraint(x, pltpu.VMEM)


def made(shape):
    return jax.ShapeDtypeStruct(shape, jnp.float32) if INTERPRET else pltpu.VMEM(shape, jnp.float32)


def dot(a, b):
    return jnp.dot(a, b, precision=highest, preferred_element_type=jnp.float32)


def thirds(x):
    high = x.astype(jnp.bfloat16)
    rest = x - high.astype(jnp.float32)
    mid = rest.astype(jnp.bfloat16)
    low = (rest - mid.astype(jnp.float32)).astype(jnp.bfloat16)
    return high, mid, low


def turned(x):
    half = x.shape[1] // 2
    return jnp.concatenate([-x[:, half:], x[:, :half]], axis=1)


def tables(size, owners):
    kept, per = size // 2, size // (2 * owners)
    signed = np.arange(kept) - size // 4
    full = np.arange(size)
    angle = 2.0 * np.pi / size * (full[:, None] * signed[None, :] % size)
    cosine, sine = np.cos(angle), np.sin(angle)
    rows = [np.einsum("yb,tu->ytub", part, np.eye(per)).reshape(size * per, per * kept) for part in (cosine, sine)]
    along_y = np.concatenate(rows, axis=1)
    along_z = np.block([[cosine.T, sine.T], [-sine.T, cosine.T]])
    along_x = np.block([[cosine, -sine], [sine, cosine]])
    own = size // owners
    back = [part.reshape(owners, own * per, per * kept).transpose(2, 1, 0).reshape(per * kept, size * per) for part in rows]
    back_y = np.concatenate([back[0], -back[1]], axis=1)
    as32 = lambda x: np.asarray(x, np.float32)
    return as32(along_y), as32(along_z), as32(along_x), as32(along_x.T), as32(along_z.T / size**3), as32(back_y)


def places(points, size, owners):
    quarter = size // 4
    plane = (points // (size * size) + quarter) % size
    row = (points // size + quarter) % size
    column = (points + quarter) % size
    return plane // owners * (size // 2) + row, column


def picks(index, count):
    return lax.broadcasted_iota(jnp.int32, (count, index.shape[1]), 0) == index


def own_points(owner_ref, points_ref, held_ref, sem):
    copy = pltpu.make_async_copy(points_ref.at[owner_ref[0]], held_ref, sem)
    copy.start()
    copy.wait()
    return held_ref[...]


def spread_kernel(owner_ref, psi_ref, points_ref, along_ref, out_ref, held_ref, sem, *, size, owners):
    line, column = places(own_points(owner_ref, points_ref, held_ref, sem), size, owners)
    at_line = picks(line, along_ref.shape[1] // 2).astype(jnp.bfloat16)
    at_column = picks(column, size // 2)
    zero = jnp.zeros((), jnp.bfloat16)
    total = None
    for real, imag in zip(thirds(psi_ref[0]), thirds(psi_ref[1])):
        spread = jnp.concatenate([jnp.where(at_column, real, zero), jnp.where(at_column, imag, zero)], axis=0)
        term = lax.dot_general(at_line, spread, (((1,), (1,)), ((), ())), preferred_element_type=jnp.float32)
        total = term if total is None else total + term
    out_ref[...] = dot(along_ref[...], jnp.concatenate([total, turned(total)], axis=0))


def fan_kernel(rows_ref, psi_ref, out_ref):
    for i in range(out_ref.shape[0]):
        out_ref[i, : rows_ref.shape[0]] = rows_ref[...]
        out_ref[i, rows_ref.shape[0] :] = psi_ref[...]


def apply_kernel(field_ref, potential_ref, z_ref, x_ref, back_x_ref, back_z_ref, out_ref, wide_ref, *, size, owners):
    per, own = size // (2 * owners), size // owners
    group = per * own
    wide = dot(field_ref[...], z_ref[...])
    for part in range(2):
        wide_ref[part] = wide[:, part * size : (part + 1) * size]

    def planes(y, part):
        return [wide_ref[part, pl.ds(y * per + t, owners, stride=group), :] for t in range(per)]

    columns = [jnp.concatenate(planes(y, 0) + planes(y, 1), axis=0) for y in range(own)]
    wave = dot(x_ref[...], jnp.concatenate(columns, axis=1))
    scale = jnp.concatenate([potential_ref[:, y, :] for y in range(own)], axis=1)
    product = jnp.concatenate([wave[:size] * scale, wave[size:] * scale], axis=0)
    back = dot(back_x_ref[...], product)
    for y in range(own):
        for t in range(per):
            for part in range(2):
                first = (part * per + t) * owners
                wide_ref[part, pl.ds(y * per + t, owners, stride=group), :] = back[first : first + owners, y * size : (y + 1) * size]
    out_ref[...] = dot(wide_ref[0], back_z_ref[:size]) + dot(wide_ref[1], back_z_ref[size:])


def pair_kernel(mine_ref, theirs_ref, product_ref, out_ref, *, owners):
    lanes = product_ref.shape[1]
    group = product_ref.shape[0] // owners
    product = product_ref[...]
    half = lanes // 2
    crossed = jnp.concatenate([product[:, half:], -product[:, :half]], axis=1)
    sums = []
    for other in (product, crossed):
        for fields_ref in (mine_ref, theirs_ref):
            for m in range(fields_ref.shape[0]):
                fields = fields_ref[m, :owners].reshape(product.shape)
                sums.append(jnp.sum(fields * other, axis=0, keepdims=True))
    sums = jnp.concatenate(sums, axis=0)
    sums = dot(sums, jnp.ones((lanes, lanes), jnp.float32))
    on_diagonal = lax.broadcasted_iota(jnp.int32, sums.shape, 0) == lax.broadcasted_iota(jnp.int32, sums.shape, 1)
    row = jnp.sum(jnp.where(on_diagonal, sums, 0.0), axis=0, keepdims=True)
    for r in range(group):
        out_ref[pl.ds(r, owners, stride=group + 1), :] = product_ref[pl.ds(r, owners, stride=group), :]
    out_ref[pl.ds(group, owners, stride=group + 1), :] = jnp.broadcast_to(row, (owners, lanes))


def project_kernel(owner_ref, core_ref, occupied_ref, rows_ref, mine_ref, theirs_ref, points_ref, along_ref, out_ref, held_ref, sem, *, size, owners, coefs):
    chips = mine_ref.shape[0]
    bands = 2 * chips
    group = rows_ref.shape[0] // owners
    sums = jnp.sum(rows_ref[pl.ds(group - 1, owners, stride=group), :], axis=0, keepdims=True)
    rows = jnp.concatenate([rows_ref[pl.ds(r, owners, stride=group), :] for r in range(group - 1)], axis=0)
    lines = dot(along_ref[...], jnp.concatenate([rows, turned(rows)], axis=0))
    line, column = places(own_points(owner_ref, points_ref, held_ref, sem), size, owners)
    at_line = picks(line, lines.shape[0]).astype(jnp.bfloat16)
    at_column = picks(column, size // 2)
    found = None
    for part in thirds(lines.T):
        term = jnp.dot(part, at_line, preferred_element_type=jnp.float32)
        found = term if found is None else found + term
    half = size // 2
    applied = [jnp.sum(jnp.where(at_column, found[p * half : (p + 1) * half], 0.0), axis=0, keepdims=True) for p in range(2)]
    tall, lanes = out_ref.shape[1:]
    taken = [jnp.zeros((tall, lanes), jnp.float32) for _ in range(2)]
    core = core_ref[0]
    for m in range(bands):
        held, chip = (mine_ref, m) if m < chips else (theirs_ref, m - chips)
        share = occupied_ref[2 * chip + (core if m < chips else 1 - core)].astype(jnp.float32)
        weight_real = sums[:, m : m + 1] * (1.0 / coefs) * share
        weight_imag = sums[:, bands + m : bands + m + 1] * (1.0 / coefs) * share
        basis = held[chip, owners:].reshape(2, tall, lanes)
        taken[0] = taken[0] + weight_real * basis[0] - weight_imag * basis[1]
        taken[1] = taken[1] + weight_imag * basis[0] + weight_real * basis[1]
    for p in range(2):
        for r in range(tall):
            out_ref[p, r : r + 1, :] = applied[p][:, r * lanes : (r + 1) * lanes] - taken[p][r : r + 1]


SCALARS = pl.BlockSpec(memory_space=pltpu.SMEM)
FAR = pl.BlockSpec(memory_space=pl.ANY)
WHOLE = pl.BlockSpec(memory_space=pltpu.VMEM)


def spread(owner, psi, points, table, size, owners):
    return pl.pallas_call(
        functools.partial(spread_kernel, size=size, owners=owners),
        out_shape=made((table.shape[0], size)),
        in_specs=[SCALARS, WHOLE, FAR, WHOLE],
        scratch_shapes=[pltpu.VMEM(points.shape[1:], points.dtype), pltpu.SemaphoreType.DMA],
        interpret=INTERPRET,
        name="spread",
    )(owner, near(psi), points, near(table))


def fan(rows, psi, copies):
    return pl.pallas_call(
        fan_kernel,
        out_shape=made((copies, rows.shape[0] + psi.shape[0], *rows.shape[1:])),
        interpret=INTERPRET,
        name="fan",
    )(near(rows), near(psi))


def apply(field, potential, along_z, along_x, back_x, back_z, size, owners):
    return pl.pallas_call(
        functools.partial(apply_kernel, size=size, owners=owners),
        out_shape=made(field.shape),
        scratch_shapes=[pltpu.VMEM((2, *field.shape), jnp.float32)],
        interpret=INTERPRET,
        name="apply",
    )(*map(near, (field, potential, along_z, along_x, back_x, back_z)))


def pair(mine, theirs, product, owners):
    return pl.pallas_call(
        functools.partial(pair_kernel, owners=owners),
        out_shape=made((product.shape[0] + owners, product.shape[1])),
        interpret=INTERPRET,
        name="pair",
    )(*map(near, (mine, theirs, product)))


def project(at, occupied, rows, mine, theirs, points, table, size, owners, coefs):
    block = points.shape[2]
    return pl.pallas_call(
        functools.partial(project_kernel, size=size, owners=owners, coefs=coefs),
        out_shape=jax.ShapeDtypeStruct((2, block // size, size), jnp.float32),
        in_specs=[SCALARS, SCALARS, SCALARS, WHOLE, WHOLE, WHOLE, FAR, WHOLE],
        scratch_shapes=[pltpu.VMEM(points.shape[1:], points.dtype), pltpu.SemaphoreType.DMA],
        interpret=INTERPRET,
        name="project",
    )(*at, occupied, near(rows), near(mine), near(theirs), points, near(table))


def shards(psi, potential, miller, occupied):
    size = potential.shape[0]
    owners = lax.axis_size("ga")
    block = psi.shape[2]
    along_y, along_z, along_x, back_x, back_z, back_y = tables(size, owners)
    at = tuple(lax.axis_index(axis).reshape(1) for axis in ("ga", "core"))
    points = miller.reshape(-1, 1, block)
    rows = spread(at[0], psi, points, along_y, size, owners)
    group = rows.shape[0] // owners
    rows = lax.all_to_all(rows.reshape(owners, group, size), "ga", split_axis=0, concat_axis=0, tiled=True)
    sent = fan(rows, psi.reshape(-1, group, size), lax.axis_size("chip"))
    mine = lax.all_to_all(sent, "chip", split_axis=0, concat_axis=0, tiled=True)
    theirs = lax.ppermute(mine, "core", [(0, 1), (1, 0)])
    product = apply(rows.reshape(-1, size), potential, along_z, along_x, back_x, back_z, size, owners)
    rows = pair(mine, theirs, product, owners)
    rows = lax.all_to_all(rows.reshape(owners, 1, -1), "ga", split_axis=0, concat_axis=0, tiled=True).reshape(rows.shape)
    out = project(at, occupied, rows, mine, theirs, points, back_y, size, owners, miller.shape[0])
    return out.reshape(2, 1, block)


def solution(mesh):
    groups, owners, bands = (mesh.shape[axis] for axis in ("pert", "ga", "band"))
    mesh = Mesh(mesh.devices.reshape(groups, owners, bands // 2, 2), ("pert", "ga", "chip", "core"))
    in_specs = (P(None, ("chip", "core"), "ga"), P("pert", "ga", None), P(), P())
    out_specs = P(None, ("pert", "chip", "core"), "ga")
    return jax.shard_map(shards, mesh=mesh, in_specs=in_specs, out_specs=out_specs, check_vma=False)
```

```python
import functools

import jax
import jax.numpy as jnp
import numpy as np
from jax import lax
from jax.experimental import pallas as pl
from jax.experimental.pallas import tpu as pltpu
from jax.sharding import Mesh
from jax.sharding import PartitionSpec as P

highest = lax.Precision.HIGHEST
INTERPRET = False


def near(x):
    return x if INTERPRET else pltpu.with_memory_space_constraint(x, pltpu.VMEM)


def made(shape, dtype=jnp.float32):
    return jax.ShapeDtypeStruct(shape, dtype) if INTERPRET else pltpu.VMEM(shape, dtype)


def halves(x):
    high = x.astype(jnp.bfloat16)
    return high, (x - high.astype(jnp.float32)).astype(jnp.bfloat16)


def dot(a, b):
    part = functools.partial(jnp.dot, preferred_element_type=jnp.float32)
    return part(a[0], b[0]) + (part(a[0], b[1]) + part(a[1], b[0]))


def turned(x):
    half = x.shape[1] // 2
    return jnp.concatenate([-x[:, half:], x[:, :half]], axis=1)


def tables(size, owners):
    signed = np.arange(size // 2) - size // 4
    angle = 2.0 * np.pi / size * (np.arange(size)[:, None] * signed[None, :] % size)
    cosine, sine = np.cos(angle), np.sin(angle)
    along_y = np.concatenate([cosine, sine], axis=1)
    along_z = np.block([[cosine.T, sine.T], [-sine.T, cosine.T]])
    along_x = np.block([[cosine, -sine], [sine, cosine]])
    back = [part.reshape(owners, size // owners, -1).transpose(2, 1, 0).reshape(size // 2, size) for part in (cosine, -sine)]
    back_y = np.concatenate(back, axis=1)

    def both(table):
        table = np.asarray(table, np.float32)
        high = table.astype(jnp.bfloat16)
        return np.stack([high, (table - high.astype(np.float32)).astype(jnp.bfloat16)])

    return tuple(map(both, (along_y, along_z, along_x, along_x.T, along_z.T / size**3, back_y)))


def places(points, size, owners):
    quarter = size // 4
    plane = (points // (size * size) + quarter) % size
    row = (points // size + quarter) % size
    column = (points + quarter) % size
    return plane // owners * (size // 2) + row, column


def picks(index, count):
    return lax.broadcasted_iota(jnp.int32, (count, index.shape[1]), 0) == index


def own_points(owner_ref, points_ref, held_ref, sem):
    return pltpu.make_async_copy(points_ref.at[owner_ref[0]], held_ref, sem)


def spread_kernel(owner_ref, psi_ref, points_ref, along_ref, out_ref, psi_held, points_held, along_held, sems, *, size, owners):
    copies = [
        own_points(owner_ref, points_ref, points_held, sems.at[0]),
        pltpu.make_async_copy(psi_ref, psi_held, sems.at[1]),
        pltpu.make_async_copy(along_ref, along_held, sems.at[2]),
    ]
    for copy in copies:
        copy.start()
    copies[0].wait()
    line, column = places(points_held[...], size, owners)
    half = size // 2
    lines = half * half // owners
    at_line = picks(line, lines).astype(jnp.bfloat16)
    at_column = picks(column, half)
    zero = jnp.zeros((), jnp.bfloat16)
    copies[1].wait()
    parts = [part for pair in zip(halves(psi_held[0]), halves(psi_held[1])) for part in pair]
    values = jnp.concatenate([jnp.where(at_column, part, zero) for part in parts], axis=0)
    total = lax.dot_general(at_line, values, (((1,), (1,)), ((), ())), preferred_element_type=jnp.float32)
    total = total[:, :size] + total[:, size:]
    around = turned(total)
    planes = lines // half
    fields = [jnp.concatenate([x[t * half : (t + 1) * half] for x in (total, around)], axis=0) for t in range(planes)]
    copies[2].wait()
    rows = dot(along_held[...], halves(jnp.concatenate(fields, axis=1)))
    for t in range(planes):
        out_ref[pl.ds(t, size, stride=planes), :] = rows[:, t * size : (t + 1) * size]


def fan_kernel(rows_ref, out_ref):
    for i in range(out_ref.shape[0]):
        out_ref[i] = rows_ref[...]


def apply_kernel(field_ref, potential_ref, z_ref, x_ref, back_x_ref, back_z_ref, out_ref, wide_ref, *, size, owners):
    per, own = size // (2 * owners), size // owners
    group = per * own
    wide = dot(halves(field_ref[...]), z_ref[...])
    for part in range(2):
        wide_ref[part] = wide[:, part * size : (part + 1) * size]

    def planes(y, part):
        return [wide_ref[part, pl.ds(y * per + t, owners, stride=group), :] for t in range(per)]

    columns = [jnp.concatenate(planes(y, 0) + planes(y, 1), axis=0) for y in range(own)]
    wave = dot(x_ref[...], halves(jnp.concatenate(columns, axis=1)))
    scale = jnp.concatenate([potential_ref[:, y, :] for y in range(own)], axis=1)
    product = jnp.concatenate([wave[:size] * scale, wave[size:] * scale], axis=0)
    back = dot(back_x_ref[...], halves(product))
    for y in range(own):
        for t in range(per):
            for part in range(2):
                first = (part * per + t) * owners
                wide_ref[part, pl.ds(y * per + t, owners, stride=group), :] = back[first : first + owners, y * size : (y + 1) * size]
    out_ref[...] = dot(halves(jnp.concatenate([wide_ref[0], wide_ref[1]], axis=1)), back_z_ref[...])


def pair_kernel(mine_ref, theirs_ref, product_ref, out_ref, *, owners):
    lanes = product_ref.shape[1]
    group = product_ref.shape[0] // owners
    product = product_ref[...]
    half = lanes // 2
    crossed = jnp.concatenate([product[:, half:], -product[:, :half]], axis=1)
    sums = []
    for other in (product, crossed):
        for fields_ref in (mine_ref, theirs_ref):
            for m in range(fields_ref.shape[0]):
                sums.append(jnp.sum(fields_ref[m].reshape(product.shape) * other, axis=0, keepdims=True))
    sums = jnp.concatenate(sums, axis=0)
    sums = jnp.dot(sums, jnp.ones((lanes, lanes), jnp.float32), precision=highest, preferred_element_type=jnp.float32)
    on_diagonal = lax.broadcasted_iota(jnp.int32, sums.shape, 0) == lax.broadcasted_iota(jnp.int32, sums.shape, 1)
    row = jnp.sum(jnp.where(on_diagonal, sums, 0.0), axis=0, keepdims=True)
    for r in range(group):
        out_ref[pl.ds(r, owners, stride=group + 1), :] = product_ref[pl.ds(r, owners, stride=group), :]
    out_ref[pl.ds(group, owners, stride=group + 1), :] = jnp.broadcast_to(row, (owners, lanes))


def sift_kernel(owner_ref, points_ref, after_ref, line_ref, column_ref, held_ref, sem, *, size, owners):
    del after_ref
    copy = own_points(owner_ref, points_ref, held_ref, sem)
    copy.start()
    copy.wait()
    line, column = places(held_ref[...], size, owners)
    line_ref[...] = picks(line, line_ref.shape[0]).astype(jnp.bfloat16)
    column_ref[...] = jnp.broadcast_to(column, column_ref.shape)


def project_kernel(chip_ref, core_ref, occupied_ref, rows_ref, line_ref, column_ref, along_ref, mine_ref, theirs_ref, out_ref, *, size, owners, coefs):
    chips = mine_ref.shape[0]
    bands = 2 * chips
    half = size // 2
    group = rows_ref.shape[0] // owners
    planes = line_ref.shape[0] // half
    sums = jnp.sum(rows_ref[pl.ds(group - 1, owners, stride=group), :], axis=0, keepdims=True)
    fields = []
    for t in range(planes):
        rows = [rows_ref[pl.ds(r, owners, stride=group), :] for r in range(t, group - 1, planes)]
        rows = jnp.concatenate(rows, axis=0)
        fields.append(jnp.concatenate([rows, turned(rows)], axis=0))
    lines = dot(along_ref[...], halves(jnp.concatenate(fields, axis=1)))
    lines = jnp.concatenate([lines[:, t * size : (t + 1) * size].T for t in range(planes)], axis=1)
    at_line = line_ref[...]
    found = jnp.dot(jnp.concatenate(halves(lines), axis=1), jnp.concatenate([at_line, at_line], axis=0), preferred_element_type=jnp.float32)
    at_column = picks(column_ref[:1], half)
    applied = [jnp.sum(jnp.where(at_column, found[p * half : (p + 1) * half], 0.0), axis=0, keepdims=True) for p in range(2)]
    tall, lanes = out_ref.shape[1:]
    taken = [jnp.zeros((tall, lanes), jnp.float32) for _ in range(2)]
    chip, core = chip_ref[0], core_ref[0]
    for m in range(bands):
        held, source, from_core = (mine_ref, m, core) if m < chips else (theirs_ref, m - chips, 1 - core)
        share = occupied_ref[2 * source + from_core].astype(jnp.float32) * (1.0 / coefs)
        weight_real = sums[:, m : m + 1] * share
        weight_imag = sums[:, bands + m : bands + m + 1] * share
        basis = held[lax.rem(chip + chips - source, chips)].reshape(2, tall, lanes)
        taken[0] = taken[0] + weight_real * basis[0] - weight_imag * basis[1]
        taken[1] = taken[1] + weight_imag * basis[0] + weight_real * basis[1]
    for p in range(2):
        for r in range(tall):
            out_ref[p, r : r + 1, :] = applied[p][:, r * lanes : (r + 1) * lanes] - taken[p][r : r + 1]


def carry_kernel(x_ref, after_ref, out_ref):
    del after_ref
    out_ref[...] = x_ref[...]


def join_kernel(*refs):
    for i, ref in enumerate(refs[:-1]):
        refs[-1][i] = ref[...]


SCALARS = pl.BlockSpec(memory_space=pltpu.SMEM)
FAR = pl.BlockSpec(memory_space=pl.ANY)
WHOLE = pl.BlockSpec(memory_space=pltpu.VMEM)


def spread(owner, psi, points, table, size, owners):
    return pl.pallas_call(
        functools.partial(spread_kernel, size=size, owners=owners),
        out_shape=made((size * (size // (2 * owners)), size)),
        in_specs=[SCALARS, FAR, FAR, FAR],
        scratch_shapes=[
            pltpu.VMEM(psi.shape, psi.dtype),
            pltpu.VMEM(points.shape[1:], points.dtype),
            pltpu.VMEM(table.shape, table.dtype),
            pltpu.SemaphoreType.DMA((3,)),
        ],
        interpret=INTERPRET,
        name="spread",
    )(owner, psi, points, table)


def fan(rows, copies):
    return pl.pallas_call(fan_kernel, out_shape=made((copies, *rows.shape)), interpret=INTERPRET, name="fan")(near(rows))


def carry(x, after):
    return pl.pallas_call(carry_kernel, out_shape=made(x.shape), in_specs=[WHOLE, FAR], interpret=INTERPRET, name="carry")(near(x), after)


def join(parts):
    return pl.pallas_call(join_kernel, out_shape=made((len(parts), *parts[0].shape)), interpret=INTERPRET, name="join")(*map(near, parts))


def sift(owner, points, after, size, owners):
    block = points.shape[2]
    lines = size // 2 * (size // (2 * owners))
    return pl.pallas_call(
        functools.partial(sift_kernel, size=size, owners=owners),
        out_shape=(made((lines, block), jnp.bfloat16), made((8, block), jnp.int32)),
        in_specs=[SCALARS, FAR, FAR],
        scratch_shapes=[pltpu.VMEM(points.shape[1:], points.dtype), pltpu.SemaphoreType.DMA],
        interpret=INTERPRET,
        name="sift",
    )(owner, points, after)


def apply(field, potential, along_z, along_x, back_x, back_z, size, owners):
    return pl.pallas_call(
        functools.partial(apply_kernel, size=size, owners=owners),
        out_shape=made(field.shape),
        scratch_shapes=[pltpu.VMEM((2, *field.shape), jnp.float32)],
        interpret=INTERPRET,
        name="apply",
    )(*map(near, (field, potential, along_z, along_x, back_x, back_z)))


def pair(mine, theirs, product, owners):
    return pl.pallas_call(
        functools.partial(pair_kernel, owners=owners),
        out_shape=made((product.shape[0] + owners, product.shape[1])),
        interpret=INTERPRET,
        name="pair",
    )(*map(near, (mine, theirs, product)))


def project(place, occupied, rows, picked, table, mine, theirs, size, owners, coefs):
    lanes = size
    tall = mine.shape[1] // 2
    return pl.pallas_call(
        functools.partial(project_kernel, size=size, owners=owners, coefs=coefs),
        out_shape=jax.ShapeDtypeStruct((2, tall, lanes), jnp.float32),
        in_specs=[SCALARS, SCALARS, SCALARS] + [WHOLE] * 6,
        interpret=INTERPRET,
        name="project",
    )(*place, occupied, *map(near, (rows, *picked, table, mine, theirs)))


def along_ring(x, axis, step):
    count = lax.axis_size(axis)
    return lax.ppermute(x, axis, [(i, (i + step) % count) for i in range(count)])


def shards(psi, potential, miller, occupied):
    size = potential.shape[0]
    owners, chips = lax.axis_size("ga"), lax.axis_size("chip")
    block = psi.shape[2]
    along_y, along_z, along_x, back_x, back_z, back_y = tables(size, owners)
    owner = lax.axis_index("ga").reshape(1)
    place = tuple(lax.axis_index(axis).reshape(1) for axis in ("chip", "core"))
    points = miller.reshape(-1, 1, block)
    rows = spread(owner, psi, points, along_y, size, owners)
    group = rows.shape[0] // owners
    rows = lax.all_to_all(rows.reshape(owners, group, size), "ga", split_axis=0, concat_axis=0, tiled=True)
    mine = lax.all_to_all(fan(rows, chips), "chip", split_axis=0, concat_axis=0, tiled=True)
    theirs = along_ring(mine, "core", 1)
    product = apply(rows.reshape(-1, size), potential, along_z, along_x, back_x, back_z, size, owners)
    sent = pair(mine, theirs, product, owners)
    rows = lax.all_to_all(sent.reshape(owners, 1, -1), "ga", split_axis=0, concat_axis=0, tiled=True).reshape(sent.shape)
    picked = sift(owner, points, sent, size, owners)
    own = carry(psi.reshape(-1, size), sent)
    basis = join([own] + [along_ring(own, "chip", step) for step in range(1, chips)])
    other_basis = along_ring(basis, "core", 1)
    out = project(place, occupied, rows, picked, back_y, basis, other_basis, size, owners, miller.shape[0])
    return out.reshape(2, 1, block)


def solution(mesh):
    groups, owners, bands = (mesh.shape[axis] for axis in ("pert", "ga", "band"))
    mesh = Mesh(mesh.devices.reshape(groups, owners, bands // 2, 2), ("pert", "ga", "chip", "core"))
    in_specs = (P(None, ("chip", "core"), "ga"), P("pert", "ga", None), P(), P())
    out_specs = P(None, ("pert", "chip", "core"), "ga")
    return jax.shard_map(shards, mesh=mesh, in_specs=in_specs, out_specs=out_specs, check_vma=False)
```

```python
import functools

import jax
import jax.numpy as jnp
import numpy as np
from jax import lax
from jax.experimental import pallas as pl
from jax.experimental.pallas import tpu as pltpu
from jax.sharding import Mesh
from jax.sharding import PartitionSpec as P

highest = lax.Precision.HIGHEST
INTERPRET = False


def near(x):
    return x if INTERPRET else pltpu.with_memory_space_constraint(x, pltpu.VMEM)


def made(shape, dtype=jnp.float32):
    return jax.ShapeDtypeStruct(shape, dtype) if INTERPRET else pltpu.VMEM(shape, dtype)


def halves(x):
    high = x.astype(jnp.bfloat16)
    return high, (x - high.astype(jnp.float32)).astype(jnp.bfloat16)


def dot(a, b):
    part = functools.partial(jnp.dot, preferred_element_type=jnp.float32)
    return part(a[0], b[0]) + (part(a[0], b[1]) + part(a[1], b[0]))


def turned(x):
    half = x.shape[1] // 2
    return jnp.concatenate([-x[:, half:], x[:, :half]], axis=1)


def tables(size, owners):
    signed = np.arange(size // 2) - size // 4
    angle = 2.0 * np.pi / size * (np.arange(size)[:, None] * signed[None, :] % size)
    cosine, sine = np.cos(angle), np.sin(angle)
    along_y = np.concatenate([cosine, sine], axis=1)
    along_z = np.block([[cosine.T, sine.T], [-sine.T, cosine.T]])
    along_x = np.block([[cosine, -sine], [sine, cosine]])
    back = [part.reshape(owners, size // owners, -1).transpose(2, 1, 0).reshape(size // 2, size) for part in (cosine, -sine)]
    back_y = np.concatenate(back, axis=1)

    def both(table):
        table = np.asarray(table, np.float32)
        high = table.astype(jnp.bfloat16)
        return np.stack([high, (table - high.astype(np.float32)).astype(jnp.bfloat16)])

    return tuple(map(both, (along_y, along_z, along_x, along_x.T, along_z.T / size**3, back_y)))


def places(points, size, owners):
    quarter = size // 4
    plane = (points // (size * size) + quarter) % size
    row = (points // size + quarter) % size
    column = (points + quarter) % size
    return plane // owners * (size // 2) + row, column


def picks(index, count):
    return lax.broadcasted_iota(jnp.int32, (count, index.shape[1]), 0) == index


def own_points(owner_ref, points_ref, held_ref, sem):
    return pltpu.make_async_copy(points_ref.at[owner_ref[0]], held_ref, sem)


def spread_kernel(owner_ref, core_ref, psi_ref, points_ref, along_ref, out_ref, psi_held, points_held, along_held, sems, *, size, owners):
    del core_ref
    copies = [
        own_points(owner_ref, points_ref, points_held, sems.at[0]),
        pltpu.make_async_copy(psi_ref, psi_held, sems.at[1]),
        pltpu.make_async_copy(along_ref, along_held, sems.at[2]),
    ]
    for copy in copies:
        copy.start()
    copies[0].wait()
    line, column = places(points_held[...], size, owners)
    half = size // 2
    lines = half * half // owners
    at_line = picks(line, lines).astype(jnp.bfloat16)
    at_column = picks(column, half)
    zero = jnp.zeros((), jnp.bfloat16)
    copies[1].wait()
    parts = [part for pair in zip(halves(psi_held[0]), halves(psi_held[1])) for part in pair]
    values = jnp.concatenate([jnp.where(at_column, part, zero) for part in parts], axis=0)
    total = lax.dot_general(at_line, values, (((1,), (1,)), ((), ())), preferred_element_type=jnp.float32)
    total = total[:, :size] + total[:, size:]
    around = turned(total)
    planes = lines // half
    fields = [jnp.concatenate([x[t * half : (t + 1) * half] for x in (total, around)], axis=0) for t in range(planes)]
    copies[2].wait()
    rows = dot(along_held[...], halves(jnp.concatenate(fields, axis=1)))
    for t in range(planes):
        out_ref[pl.ds(t, size, stride=planes), :] = rows[:, t * size : (t + 1) * size]


def fan_kernel(rows_ref, psi_ref, out_ref):
    for i in range(out_ref.shape[0]):
        out_ref[i, : rows_ref.shape[0]] = rows_ref[...]
        out_ref[i, rows_ref.shape[0] :] = psi_ref[...]


def apply_kernel(field_ref, potential_ref, z_ref, x_ref, back_x_ref, back_z_ref, mine_ref, out_ref, sums_ref, wide_ref, *, size, owners):
    per, own = size // (2 * owners), size // owners
    group = per * own
    wide = dot(halves(field_ref[...]), z_ref[...])
    for part in range(2):
        wide_ref[part] = wide[:, part * size : (part + 1) * size]

    def planes(y, part):
        return [wide_ref[part, pl.ds(y * per + t, owners, stride=group), :] for t in range(per)]

    columns = [jnp.concatenate(planes(y, 0) + planes(y, 1), axis=0) for y in range(own)]
    wave = dot(x_ref[...], halves(jnp.concatenate(columns, axis=1)))
    scale = jnp.concatenate([potential_ref[:, y, :] for y in range(own)], axis=1)
    product = jnp.concatenate([wave[:size] * scale, wave[size:] * scale], axis=0)
    back = dot(back_x_ref[...], halves(product))
    for y in range(own):
        for t in range(per):
            for part in range(2):
                first = (part * per + t) * owners
                wide_ref[part, pl.ds(y * per + t, owners, stride=group), :] = back[first : first + owners, y * size : (y + 1) * size]
    product = dot(halves(jnp.concatenate([wide_ref[0], wide_ref[1]], axis=1)), back_z_ref[...])
    out_ref[...] = product
    sums_ref[...] = overlaps(mine_ref, product, owners)


def overlaps(fields_ref, product, owners):
    half = product.shape[1] // 2
    crossed = jnp.concatenate([product[:, half:], -product[:, :half]], axis=1)
    fields = [fields_ref[m, :owners].reshape(product.shape) for m in range(fields_ref.shape[0])]
    return jnp.concatenate([jnp.sum(f * other, axis=0, keepdims=True) for other in (product, crossed) for f in fields], axis=0)


def pair_kernel(theirs_ref, product_ref, sums_ref, out_ref, *, owners):
    lanes = product_ref.shape[1]
    group = product_ref.shape[0] // owners
    sums = jnp.concatenate([sums_ref[...], overlaps(theirs_ref, product_ref[...], owners)], axis=0)
    sums = jnp.dot(sums, jnp.ones((lanes, lanes), jnp.float32), precision=highest, preferred_element_type=jnp.float32)
    on_diagonal = lax.broadcasted_iota(jnp.int32, sums.shape, 0) == lax.broadcasted_iota(jnp.int32, sums.shape, 1)
    row = jnp.sum(jnp.where(on_diagonal, sums, 0.0), axis=0, keepdims=True)
    for r in range(group):
        out_ref[pl.ds(r, owners, stride=group + 1), :] = product_ref[pl.ds(r, owners, stride=group), :]
    out_ref[pl.ds(group, owners, stride=group + 1), :] = jnp.broadcast_to(row, (owners, lanes))


def project_kernel(
    owner_ref, core_ref, occupied_ref, rows_ref, points_ref, along_ref, mine_ref, theirs_ref, out_ref, held_ref, sem, *, size, owners, coefs
):
    copy = own_points(owner_ref, points_ref, held_ref, sem)
    copy.start()
    chips = mine_ref.shape[0]
    bands = 2 * chips
    half = size // 2
    group = rows_ref.shape[0] // owners
    planes = half // owners
    sums = jnp.sum(rows_ref[pl.ds(group - 1, owners, stride=group), :], axis=0, keepdims=True)
    fields = []
    for t in range(planes):
        rows = [rows_ref[pl.ds(r, owners, stride=group), :] for r in range(t, group - 1, planes)]
        rows = jnp.concatenate(rows, axis=0)
        fields.append(jnp.concatenate([rows, turned(rows)], axis=0))
    lines = dot(along_ref[...], halves(jnp.concatenate(fields, axis=1)))
    lines = jnp.concatenate([lines[:, t * size : (t + 1) * size].T for t in range(planes)], axis=1)
    copy.wait()
    line, column = places(held_ref[...], size, owners)
    at_line = picks(line, lines.shape[1]).astype(jnp.bfloat16)
    at_column = picks(column, half)
    found = jnp.dot(jnp.concatenate(halves(lines), axis=1), jnp.concatenate([at_line, at_line], axis=0), preferred_element_type=jnp.float32)
    applied = [jnp.sum(jnp.where(at_column, found[p * half : (p + 1) * half], 0.0), axis=0, keepdims=True) for p in range(2)]
    tall, lanes = out_ref.shape[1:]
    taken = [jnp.zeros((tall, lanes), jnp.float32) for _ in range(2)]
    core = core_ref[0]
    for m in range(bands):
        held, first, source, from_core = (mine_ref, 0, m, core) if m < chips else (theirs_ref, 2 * chips, m - chips, 1 - core)
        share = occupied_ref[2 * source + from_core].astype(jnp.float32) * (1.0 / coefs)
        weight_real = sums[:, first + source : first + source + 1] * share
        weight_imag = sums[:, first + chips + source : first + chips + source + 1] * share
        basis = held[source, owners:].reshape(2, tall, lanes)
        taken[0] = taken[0] + weight_real * basis[0] - weight_imag * basis[1]
        taken[1] = taken[1] + weight_imag * basis[0] + weight_real * basis[1]
    for p in range(2):
        for r in range(tall):
            out_ref[p, r : r + 1, :] = applied[p][:, r * lanes : (r + 1) * lanes] - taken[p][r : r + 1]


SCALARS = pl.BlockSpec(memory_space=pltpu.SMEM)
FAR = pl.BlockSpec(memory_space=pl.ANY)
WHOLE = pl.BlockSpec(memory_space=pltpu.VMEM)


def spread(owner, core, psi, points, table, size, owners):
    return pl.pallas_call(
        functools.partial(spread_kernel, size=size, owners=owners),
        out_shape=made((size * (size // (2 * owners)), size)),
        in_specs=[SCALARS, SCALARS, FAR, FAR, FAR],
        scratch_shapes=[
            pltpu.VMEM(psi.shape, psi.dtype),
            pltpu.VMEM(points.shape[1:], points.dtype),
            pltpu.VMEM(table.shape, table.dtype),
            pltpu.SemaphoreType.DMA((3,)),
        ],
        interpret=INTERPRET,
        name="spread",
    )(owner, core, psi, points, table)


def fan(rows, psi, copies):
    shape = (copies, rows.shape[0] + psi.shape[0], *rows.shape[1:])
    return pl.pallas_call(fan_kernel, out_shape=made(shape), interpret=INTERPRET, name="fan")(near(rows), near(psi))


def apply(field, potential, along_z, along_x, back_x, back_z, mine, size, owners):
    return pl.pallas_call(
        functools.partial(apply_kernel, size=size, owners=owners),
        out_shape=(made(field.shape), made((2 * mine.shape[0], size))),
        scratch_shapes=[pltpu.VMEM((2, *field.shape), jnp.float32)],
        interpret=INTERPRET,
        name="apply",
    )(*map(near, (field, potential, along_z, along_x, back_x, back_z, mine)))


def pair(theirs, product, sums, owners):
    return pl.pallas_call(
        functools.partial(pair_kernel, owners=owners),
        out_shape=made((product.shape[0] + owners, product.shape[1])),
        interpret=INTERPRET,
        name="pair",
    )(*map(near, (theirs, product, sums)))


def project(owner, core, occupied, rows, points, table, mine, theirs, size, owners, coefs):
    block = points.shape[2]
    return pl.pallas_call(
        functools.partial(project_kernel, size=size, owners=owners, coefs=coefs),
        out_shape=jax.ShapeDtypeStruct((2, block // size, size), jnp.float32),
        in_specs=[SCALARS, SCALARS, SCALARS, WHOLE, FAR, WHOLE, WHOLE, WHOLE],
        scratch_shapes=[pltpu.VMEM(points.shape[1:], points.dtype), pltpu.SemaphoreType.DMA],
        interpret=INTERPRET,
        name="project",
    )(owner, core, occupied, near(rows), points, near(table), near(mine), near(theirs))


def along_ring(x, axis, step):
    count = lax.axis_size(axis)
    return lax.ppermute(x, axis, [(i, (i + step) % count) for i in range(count)])


def shards(psi, potential, miller, occupied):
    size = potential.shape[0]
    owners, chips = lax.axis_size("ga"), lax.axis_size("chip")
    block = psi.shape[2]
    along_y, along_z, along_x, back_x, back_z, back_y = tables(size, owners)
    owner, core = (lax.axis_index(axis).reshape(1) for axis in ("ga", "core"))
    points = miller.reshape(-1, 1, block)
    rows = spread(owner, core, psi, points, along_y, size, owners)
    group = rows.shape[0] // owners
    rows = lax.all_to_all(rows.reshape(owners, group, size), "ga", split_axis=0, concat_axis=0, tiled=True)
    sent = fan(rows, psi.reshape(-1, group, size), chips)
    mine = lax.all_to_all(sent, "chip", split_axis=0, concat_axis=0, tiled=True)
    theirs = along_ring(mine, "core", 1)
    product, sums = apply(rows.reshape(-1, size), potential, along_z, along_x, back_x, back_z, mine, size, owners)
    sent = pair(theirs, product, sums, owners)
    rows = lax.all_to_all(sent.reshape(owners, 1, -1), "ga", split_axis=0, concat_axis=0, tiled=True).reshape(sent.shape)
    out = project(owner, core, occupied, rows, points, back_y, mine, theirs, size, owners, miller.shape[0])
    return out.reshape(2, 1, block)


def solution(mesh):
    groups, owners, bands = (mesh.shape[axis] for axis in ("pert", "ga", "band"))
    mesh = Mesh(mesh.devices.reshape(groups, owners, bands // 2, 2), ("pert", "ga", "chip", "core"))
    in_specs = (P(None, ("chip", "core"), "ga"), P("pert", "ga", None), P(), P())
    out_specs = P(None, ("pert", "chip", "core"), "ga")
    return jax.shard_map(shards, mesh=mesh, in_specs=in_specs, out_specs=out_specs, check_vma=False)
```

```python
import functools

import jax
import jax.numpy as jnp
import numpy as np
from jax import lax
from jax.experimental import pallas as pl
from jax.experimental.pallas import tpu as pltpu
from jax.sharding import Mesh
from jax.sharding import PartitionSpec as P

highest = lax.Precision.HIGHEST
INTERPRET = False


def near(x):
    return x if INTERPRET else pltpu.with_memory_space_constraint(x, pltpu.VMEM)


def made(shape, dtype=jnp.float32):
    return jax.ShapeDtypeStruct(shape, dtype) if INTERPRET else pltpu.VMEM(shape, dtype)


def halves(x):
    high = x.astype(jnp.bfloat16)
    return high, (x - high.astype(jnp.float32)).astype(jnp.bfloat16)


def dot(a, b):
    part = functools.partial(jnp.dot, preferred_element_type=jnp.float32)
    return part(a[0], b[0]) + (part(a[0], b[1]) + part(a[1], b[0]))


def turned(x):
    half = x.shape[1] // 2
    return jnp.concatenate([-x[:, half:], x[:, :half]], axis=1)


def tables(size, owners):
    signed = np.arange(size // 2) - size // 4
    angle = 2.0 * np.pi / size * (np.arange(size)[:, None] * signed[None, :] % size)
    cosine, sine = np.cos(angle), np.sin(angle)
    along_y = np.concatenate([cosine, sine], axis=1)
    along_z = np.block([[cosine.T, sine.T], [-sine.T, cosine.T]])
    along_x = np.block([[cosine, -sine], [sine, cosine]])
    back = [part.reshape(owners, size // owners, -1).transpose(2, 1, 0).reshape(size // 2, size) for part in (cosine, -sine)]
    back_y = np.concatenate(back, axis=1)

    def both(table):
        table = np.asarray(table, np.float32)
        high = table.astype(jnp.bfloat16)
        return np.stack([high, (table - high.astype(np.float32)).astype(jnp.bfloat16)])

    return tuple(map(both, (along_y, along_z, along_x, along_x.T, along_z.T / size**3, back_y)))


def places(points, size, owners):
    quarter = size // 4
    plane = (points // (size * size) + quarter) % size
    row = (points // size + quarter) % size
    column = (points + quarter) % size
    return plane // owners * (size // 2) + row, column


def own_points(owner_ref, points_ref, held_ref, sem):
    return pltpu.make_async_copy(points_ref.at[owner_ref[0]], held_ref, sem)


def numbered(count, lanes):
    return lax.broadcasted_iota(jnp.int32, (count, lanes), 0).astype(jnp.float32).astype(jnp.bfloat16)


def copied_down(row, count):
    some = jnp.broadcast_to(row, (16, row.shape[1])).astype(jnp.bfloat16)
    return jnp.concatenate([some] * (count // 16), axis=0)


def spread_kernel(
    owner_ref, core_ref, psi_ref, points_ref, along_ref, out_ref, psi_held, points_held, along_held, flat_ref, sems, *, size, owners
):
    del core_ref
    copies = [
        own_points(owner_ref, points_ref, points_held, sems.at[0]),
        pltpu.make_async_copy(psi_ref, psi_held, sems.at[1]),
        pltpu.make_async_copy(along_ref, along_held, sems.at[2]),
    ]
    for copy in copies:
        copy.start()
    half = size // 2
    lines = half * half // owners
    copies[0].wait()
    line, column = places(points_held[...], size, owners)
    flat_ref[0], flat_ref[1] = line.astype(jnp.float32), column.astype(jnp.float32)
    copies[1].wait()
    for part in range(2):
        for which, x in enumerate(halves(psi_held[part])):
            flat_ref[2 + 2 * which + part] = x.astype(jnp.float32)
    tall, lanes = points_held.shape
    every_line, every_column = numbered(lines, lanes), numbered(half, lanes)
    one, zero = jnp.ones((), jnp.bfloat16), jnp.zeros((), jnp.bfloat16)
    at_line, values = [], []
    for r in range(tall):
        at_line.append(jnp.where(every_line == copied_down(flat_ref[0, r : r + 1, :], lines), one, zero))
        at_column = every_column == copied_down(flat_ref[1, r : r + 1, :], half)
        parts = [jnp.where(at_column, copied_down(flat_ref[i, r : r + 1, :], half), zero) for i in range(2, 6)]
        values.append(jnp.concatenate(parts, axis=0))
    at_line, values = jnp.concatenate(at_line, axis=1), jnp.concatenate(values, axis=1)
    total = lax.dot_general(at_line, values, (((1,), (1,)), ((), ())), preferred_element_type=jnp.float32)
    total = total[:, :size] + total[:, size:]
    around = turned(total)
    planes = lines // half
    fields = [jnp.concatenate([x[t * half : (t + 1) * half] for x in (total, around)], axis=0) for t in range(planes)]
    copies[2].wait()
    rows = dot(along_held[...], halves(jnp.concatenate(fields, axis=1)))
    for t in range(planes):
        out_ref[pl.ds(t, size, stride=planes), :] = rows[:, t * size : (t + 1) * size]


def fan_kernel(rows_ref, psi_ref, out_ref):
    for i in range(out_ref.shape[0]):
        out_ref[i, : rows_ref.shape[0]] = rows_ref[...]
        out_ref[i, rows_ref.shape[0] :] = psi_ref[...]


def apply_kernel(field_ref, potential_ref, z_ref, x_ref, back_x_ref, back_z_ref, mine_ref, out_ref, sums_ref, wide_ref, *, size, owners):
    per, own = size // (2 * owners), size // owners
    group = per * own
    wide = dot(halves(field_ref[...]), z_ref[...])
    for part in range(2):
        wide_ref[part] = wide[:, part * size : (part + 1) * size]

    def planes(y, part):
        return [wide_ref[part, pl.ds(y * per + t, owners, stride=group), :] for t in range(per)]

    columns = [jnp.concatenate(planes(y, 0) + planes(y, 1), axis=0) for y in range(own)]
    wave = dot(x_ref[...], halves(jnp.concatenate(columns, axis=1)))
    scale = jnp.concatenate([potential_ref[:, y, :] for y in range(own)], axis=1)
    product = jnp.concatenate([wave[:size] * scale, wave[size:] * scale], axis=0)
    back = dot(back_x_ref[...], halves(product))
    for y in range(own):
        for t in range(per):
            for part in range(2):
                first = (part * per + t) * owners
                wide_ref[part, pl.ds(y * per + t, owners, stride=group), :] = back[first : first + owners, y * size : (y + 1) * size]
    product = dot(halves(jnp.concatenate([wide_ref[0], wide_ref[1]], axis=1)), back_z_ref[...])
    out_ref[...] = product
    sums_ref[...] = overlaps(mine_ref, product, owners)


def overlaps(fields_ref, product, owners):
    half = product.shape[1] // 2
    crossed = jnp.concatenate([product[:, half:], -product[:, :half]], axis=1)
    fields = [fields_ref[m, :owners].reshape(product.shape) for m in range(fields_ref.shape[0])]
    return jnp.concatenate([jnp.sum(f * other, axis=0, keepdims=True) for other in (product, crossed) for f in fields], axis=0)


def pair_kernel(theirs_ref, product_ref, sums_ref, out_ref, *, owners):
    lanes = product_ref.shape[1]
    group = product_ref.shape[0] // owners
    sums = jnp.concatenate([sums_ref[...], overlaps(theirs_ref, product_ref[...], owners)], axis=0)
    sums = jnp.dot(sums, jnp.ones((lanes, lanes), jnp.float32), precision=highest, preferred_element_type=jnp.float32)
    on_diagonal = lax.broadcasted_iota(jnp.int32, sums.shape, 0) == lax.broadcasted_iota(jnp.int32, sums.shape, 1)
    row = jnp.sum(jnp.where(on_diagonal, sums, 0.0), axis=0, keepdims=True)
    for r in range(group):
        out_ref[pl.ds(r, owners, stride=group + 1), :] = product_ref[pl.ds(r, owners, stride=group), :]
    out_ref[pl.ds(group, owners, stride=group + 1), :] = jnp.broadcast_to(row, (owners, lanes))


def project_kernel(
    owner_ref, core_ref, occupied_ref, rows_ref, points_ref, along_ref, mine_ref, theirs_ref, out_ref, held_ref, flat_ref, sem, *, size, owners, coefs
):
    copy = own_points(owner_ref, points_ref, held_ref, sem)
    copy.start()
    chips = mine_ref.shape[0]
    bands = 2 * chips
    half = size // 2
    group = rows_ref.shape[0] // owners
    planes = half // owners
    sums = jnp.sum(rows_ref[pl.ds(group - 1, owners, stride=group), :], axis=0, keepdims=True)
    fields = []
    for t in range(planes):
        rows = [rows_ref[pl.ds(r, owners, stride=group), :] for r in range(t, group - 1, planes)]
        rows = jnp.concatenate(rows, axis=0)
        fields.append(jnp.concatenate([rows, turned(rows)], axis=0))
    lines = dot(along_ref[...], halves(jnp.concatenate(fields, axis=1)))
    lines = jnp.concatenate([lines[:, t * size : (t + 1) * size].T for t in range(planes)], axis=1)
    lines = jnp.concatenate(halves(lines), axis=1)
    copy.wait()
    line, column = places(held_ref[...], size, owners)
    flat_ref[0], flat_ref[1] = line.astype(jnp.float32), column.astype(jnp.float32)
    tall, lanes = out_ref.shape[1:]
    taken = [jnp.zeros((tall, lanes), jnp.float32) for _ in range(2)]
    core = core_ref[0]
    for m in range(bands):
        held, first, source, from_core = (mine_ref, 0, m, core) if m < chips else (theirs_ref, 2 * chips, m - chips, 1 - core)
        share = occupied_ref[2 * source + from_core].astype(jnp.float32) * (1.0 / coefs)
        weight_real = sums[:, first + source : first + source + 1] * share
        weight_imag = sums[:, first + chips + source : first + chips + source + 1] * share
        basis = held[source, owners:].reshape(2, tall, lanes)
        taken[0] = taken[0] + weight_real * basis[0] - weight_imag * basis[1]
        taken[1] = taken[1] + weight_imag * basis[0] + weight_real * basis[1]
    every_line = numbered(planes * half, lanes)
    every_column = lax.broadcasted_iota(jnp.int32, (half, lanes), 0).astype(jnp.float32)
    one, zero = jnp.ones((), jnp.bfloat16), jnp.zeros((), jnp.bfloat16)
    for r in range(0, tall, 2):
        at_line = [jnp.where(every_line == copied_down(flat_ref[0, i : i + 1, :], planes * half), one, zero) for i in (r, r + 1)]
        at_line = jnp.concatenate(at_line, axis=1)
        found = jnp.dot(lines, jnp.concatenate([at_line, at_line], axis=0), preferred_element_type=jnp.float32)
        for i in range(2):
            at_column = every_column == flat_ref[1, r + i : r + i + 1, :]
            for p in range(2):
                applied = jnp.where(at_column, found[p * half : (p + 1) * half, i * lanes : (i + 1) * lanes], 0.0)
                out_ref[p, r + i : r + i + 1, :] = jnp.sum(applied, axis=0, keepdims=True) - taken[p][r + i : r + i + 1]


SCALARS = pl.BlockSpec(memory_space=pltpu.SMEM)
FAR = pl.BlockSpec(memory_space=pl.ANY)
WHOLE = pl.BlockSpec(memory_space=pltpu.VMEM)


def spread(owner, core, psi, points, table, size, owners):
    return pl.pallas_call(
        functools.partial(spread_kernel, size=size, owners=owners),
        out_shape=made((size * (size // (2 * owners)), size)),
        in_specs=[SCALARS, SCALARS, FAR, FAR, FAR],
        scratch_shapes=[
            pltpu.VMEM(psi.shape, psi.dtype),
            pltpu.VMEM(points.shape[1:], points.dtype),
            pltpu.VMEM(table.shape, table.dtype),
            pltpu.VMEM((6, *points.shape[1:]), jnp.float32),
            pltpu.SemaphoreType.DMA((3,)),
        ],
        interpret=INTERPRET,
        name="spread",
    )(owner, core, psi, points, table)


def fan(rows, psi, copies):
    shape = (copies, rows.shape[0] + psi.shape[0], *rows.shape[1:])
    return pl.pallas_call(fan_kernel, out_shape=made(shape), interpret=INTERPRET, name="fan")(near(rows), near(psi))


def apply(field, potential, along_z, along_x, back_x, back_z, mine, size, owners):
    return pl.pallas_call(
        functools.partial(apply_kernel, size=size, owners=owners),
        out_shape=(made(field.shape), made((2 * mine.shape[0], size))),
        scratch_shapes=[pltpu.VMEM((2, *field.shape), jnp.float32)],
        interpret=INTERPRET,
        name="apply",
    )(*map(near, (field, potential, along_z, along_x, back_x, back_z, mine)))


def pair(theirs, product, sums, owners):
    return pl.pallas_call(
        functools.partial(pair_kernel, owners=owners),
        out_shape=made((product.shape[0] + owners, product.shape[1])),
        interpret=INTERPRET,
        name="pair",
    )(*map(near, (theirs, product, sums)))


def project(owner, core, occupied, rows, points, table, mine, theirs, size, owners, coefs):
    tall, lanes = points.shape[1:]
    return pl.pallas_call(
        functools.partial(project_kernel, size=size, owners=owners, coefs=coefs),
        out_shape=jax.ShapeDtypeStruct((2, tall, lanes), jnp.float32),
        in_specs=[SCALARS, SCALARS, SCALARS, WHOLE, FAR, WHOLE, WHOLE, WHOLE],
        scratch_shapes=[pltpu.VMEM((tall, lanes), points.dtype), pltpu.VMEM((2, tall, lanes), jnp.float32), pltpu.SemaphoreType.DMA],
        interpret=INTERPRET,
        name="project",
    )(owner, core, occupied, near(rows), points, near(table), near(mine), near(theirs))


def along_ring(x, axis, step):
    count = lax.axis_size(axis)
    return lax.ppermute(x, axis, [(i, (i + step) % count) for i in range(count)])


def shards(psi, potential, miller, occupied):
    size = potential.shape[0]
    owners, chips = lax.axis_size("ga"), lax.axis_size("chip")
    block = psi.shape[2]
    along_y, along_z, along_x, back_x, back_z, back_y = tables(size, owners)
    owner, core = (lax.axis_index(axis).reshape(1) for axis in ("ga", "core"))
    points = miller.reshape(-1, block // size, size)
    rows = spread(owner, core, psi.reshape(2, -1, size), points, along_y, size, owners)
    group = rows.shape[0] // owners
    rows = lax.all_to_all(rows.reshape(owners, group, size), "ga", split_axis=0, concat_axis=0, tiled=True)
    sent = fan(rows, psi.reshape(-1, group, size), chips)
    mine = lax.all_to_all(sent, "chip", split_axis=0, concat_axis=0, tiled=True)
    theirs = along_ring(mine, "core", 1)
    product, sums = apply(rows.reshape(-1, size), potential, along_z, along_x, back_x, back_z, mine, size, owners)
    sent = pair(theirs, product, sums, owners)
    rows = lax.all_to_all(sent.reshape(owners, 1, -1), "ga", split_axis=0, concat_axis=0, tiled=True).reshape(sent.shape)
    out = project(owner, core, occupied, rows, points, back_y, mine, theirs, size, owners, miller.shape[0])
    return out.reshape(2, 1, block)


def solution(mesh):
    groups, owners, bands = (mesh.shape[axis] for axis in ("pert", "ga", "band"))
    mesh = Mesh(mesh.devices.reshape(groups, owners, bands // 2, 2), ("pert", "ga", "chip", "core"))
    in_specs = (P(None, ("chip", "core"), "ga"), P("pert", "ga", None), P(), P())
    out_specs = P(None, ("pert", "chip", "core"), "ga")
    return jax.shard_map(shards, mesh=mesh, in_specs=in_specs, out_specs=out_specs, check_vma=False)
```

```python
import functools

import jax
import jax.numpy as jnp
import numpy as np
from jax import lax
from jax.experimental import pallas as pl
from jax.experimental.pallas import tpu as pltpu
from jax.sharding import Mesh
from jax.sharding import PartitionSpec as P

highest = lax.Precision.HIGHEST
INTERPRET = False


def near(x):
    return x if INTERPRET else pltpu.with_memory_space_constraint(x, pltpu.VMEM)


def made(shape, dtype=jnp.float32):
    return jax.ShapeDtypeStruct(shape, dtype) if INTERPRET else pltpu.VMEM(shape, dtype)


def halves(x):
    high = x.astype(jnp.bfloat16)
    return high, (x - high.astype(jnp.float32)).astype(jnp.bfloat16)


def dot(a, b):
    part = functools.partial(jnp.dot, preferred_element_type=jnp.float32)
    return part(a[0], b[0]) + (part(a[0], b[1]) + part(a[1], b[0]))


def turned(x):
    half = x.shape[1] // 2
    return jnp.concatenate([-x[:, half:], x[:, :half]], axis=1)


def tables(size, owners):
    signed = np.arange(size // 2) - size // 4
    angle = 2.0 * np.pi / size * (np.arange(size)[:, None] * signed[None, :] % size)
    cosine, sine = np.cos(angle), np.sin(angle)
    along_y = np.concatenate([cosine, sine], axis=1)
    along_z = np.block([[cosine.T, sine.T], [-sine.T, cosine.T]])
    along_x = np.block([[cosine, -sine], [sine, cosine]])
    back = [part.reshape(owners, size // owners, -1).transpose(2, 1, 0).reshape(size // 2, size) for part in (cosine, -sine)]
    back_y = np.concatenate(back, axis=1)

    def both(table):
        table = np.asarray(table, np.float32)
        high = table.astype(jnp.bfloat16)
        return np.stack([high, (table - high.astype(np.float32)).astype(jnp.bfloat16)])

    return tuple(map(both, (along_y, along_z, along_x, along_x.T, along_z.T / size**3, back_y)))


def places(points, size, owners):
    quarter = size // 4
    plane = (points // (size * size) + quarter) % size
    row = (points // size + quarter) % size
    column = (points + quarter) % size
    return plane // owners * (size // 2) + row, column


def own_points(owner_ref, points_ref, held_ref, sem):
    return pltpu.make_async_copy(points_ref.at[owner_ref[0]], held_ref, sem)


def numbered(count, lanes):
    return lax.broadcasted_iota(jnp.int32, (count, lanes), 0).astype(jnp.float32).astype(jnp.bfloat16)


def copied_down(row, count):
    some = jnp.broadcast_to(row, (16, row.shape[1])).astype(jnp.bfloat16)
    return jnp.concatenate([some] * (count // 16), axis=0)


def spread_kernel(
    owner_ref, psi_ref, points_ref, along_ref, out_ref, psi_held, points_held, along_held, flat_ref, sems, *, size, owners
):
    copies = [
        own_points(owner_ref, points_ref, points_held, sems.at[0]),
        pltpu.make_async_copy(psi_ref, psi_held, sems.at[1]),
        pltpu.make_async_copy(along_ref, along_held, sems.at[2]),
    ]
    for copy in copies:
        copy.start()
    half = size // 2
    lines = half * half // owners
    copies[0].wait()
    line, column = places(points_held[...], size, owners)
    flat_ref[0], flat_ref[1] = line.astype(jnp.float32), column.astype(jnp.float32)
    copies[1].wait()
    for part in range(2):
        for which, x in enumerate(halves(psi_held[part])):
            flat_ref[2 + 2 * which + part] = x.astype(jnp.float32)
    tall, lanes = points_held.shape
    every_line, every_column = numbered(lines, lanes), numbered(half, lanes)
    one, zero = jnp.ones((), jnp.bfloat16), jnp.zeros((), jnp.bfloat16)
    at_line, values = [], []
    for r in range(tall):
        at_line.append(jnp.where(every_line == copied_down(flat_ref[0, r : r + 1, :], lines), one, zero))
        at_column = every_column == copied_down(flat_ref[1, r : r + 1, :], half)
        parts = [jnp.where(at_column, copied_down(flat_ref[i, r : r + 1, :], half), zero) for i in range(2, 6)]
        values.append(jnp.concatenate(parts, axis=0))
    at_line, values = jnp.concatenate(at_line, axis=1), jnp.concatenate(values, axis=1)
    total = lax.dot_general(at_line, values, (((1,), (1,)), ((), ())), preferred_element_type=jnp.float32)
    total = total[:, :size] + total[:, size:]
    around = turned(total)
    planes = lines // half
    fields = [jnp.concatenate([x[t * half : (t + 1) * half] for x in (total, around)], axis=0) for t in range(planes)]
    copies[2].wait()
    rows = dot(along_held[...], halves(jnp.concatenate(fields, axis=1)))
    for t in range(planes):
        out_ref[pl.ds(t, size, stride=planes), :] = rows[:, t * size : (t + 1) * size]


def fan_kernel(rows_ref, out_ref):
    for i in range(out_ref.shape[0]):
        out_ref[i] = rows_ref[...]


def carry_kernel(x_ref, after_ref, out_ref):
    del after_ref
    out_ref[...] = x_ref[...]


def join_kernel(*refs):
    for i, ref in enumerate(refs[:-1]):
        refs[-1][i] = ref[...]


def apply_kernel(field_ref, potential_ref, z_ref, x_ref, back_x_ref, back_z_ref, mine_ref, out_ref, sums_ref, wide_ref, *, size, owners):
    per, own = size // (2 * owners), size // owners
    group = per * own
    wide = dot(halves(field_ref[...]), z_ref[...])
    for part in range(2):
        wide_ref[part] = wide[:, part * size : (part + 1) * size]

    def planes(y, part):
        return [wide_ref[part, pl.ds(y * per + t, owners, stride=group), :] for t in range(per)]

    columns = [jnp.concatenate(planes(y, 0) + planes(y, 1), axis=0) for y in range(own)]
    wave = dot(x_ref[...], halves(jnp.concatenate(columns, axis=1)))
    scale = jnp.concatenate([potential_ref[:, y, :] for y in range(own)], axis=1)
    product = jnp.concatenate([wave[:size] * scale, wave[size:] * scale], axis=0)
    back = dot(back_x_ref[...], halves(product))
    for y in range(own):
        for t in range(per):
            for part in range(2):
                first = (part * per + t) * owners
                wide_ref[part, pl.ds(y * per + t, owners, stride=group), :] = back[first : first + owners, y * size : (y + 1) * size]
    product = dot(halves(jnp.concatenate([wide_ref[0], wide_ref[1]], axis=1)), back_z_ref[...])
    out_ref[...] = product
    sums_ref[...] = overlaps(mine_ref, product)


def overlaps(fields_ref, product):
    half = product.shape[1] // 2
    crossed = jnp.concatenate([product[:, half:], -product[:, :half]], axis=1)
    fields = [fields_ref[m].reshape(product.shape) for m in range(fields_ref.shape[0])]
    return jnp.concatenate([jnp.sum(f * other, axis=0, keepdims=True) for other in (product, crossed) for f in fields], axis=0)


def pair_kernel(theirs_ref, product_ref, sums_ref, out_ref, *, owners):
    lanes = product_ref.shape[1]
    group = product_ref.shape[0] // owners
    sums = jnp.concatenate([sums_ref[...], overlaps(theirs_ref, product_ref[...])], axis=0)
    sums = jnp.dot(sums, jnp.ones((lanes, lanes), jnp.float32), precision=highest, preferred_element_type=jnp.float32)
    on_diagonal = lax.broadcasted_iota(jnp.int32, sums.shape, 0) == lax.broadcasted_iota(jnp.int32, sums.shape, 1)
    row = jnp.sum(jnp.where(on_diagonal, sums, 0.0), axis=0, keepdims=True)
    for r in range(group):
        out_ref[pl.ds(r, owners, stride=group + 1), :] = product_ref[pl.ds(r, owners, stride=group), :]
    out_ref[pl.ds(group, owners, stride=group + 1), :] = jnp.broadcast_to(row, (owners, lanes))


def sift_kernel(owner_ref, points_ref, after_ref, line_ref, column_ref, held_ref, flat_ref, sem, *, size, owners):
    del after_ref
    copy = own_points(owner_ref, points_ref, held_ref, sem)
    copy.start()
    copy.wait()
    line, column = places(held_ref[...], size, owners)
    flat_ref[...], column_ref[...] = line.astype(jnp.float32), column.astype(jnp.float32)
    tall, lanes = held_ref.shape
    lines = line_ref.shape[0]
    every_line = numbered(lines, lanes)
    one, zero = jnp.ones((), jnp.bfloat16), jnp.zeros((), jnp.bfloat16)
    for r in range(tall):
        line_ref[:, r * lanes : (r + 1) * lanes] = jnp.where(every_line == copied_down(flat_ref[r : r + 1, :], lines), one, zero)


def project_kernel(
    chip_ref, core_ref, occupied_ref, rows_ref, line_ref, column_ref, along_ref, mine_ref, theirs_ref, out_ref, *, size, owners, coefs
):
    chips = mine_ref.shape[0]
    bands = 2 * chips
    half = size // 2
    group = rows_ref.shape[0] // owners
    planes = half // owners
    sums = jnp.sum(rows_ref[pl.ds(group - 1, owners, stride=group), :], axis=0, keepdims=True)
    fields = []
    for t in range(planes):
        rows = [rows_ref[pl.ds(r, owners, stride=group), :] for r in range(t, group - 1, planes)]
        rows = jnp.concatenate(rows, axis=0)
        fields.append(jnp.concatenate([rows, turned(rows)], axis=0))
    lines = dot(along_ref[...], halves(jnp.concatenate(fields, axis=1)))
    lines = jnp.concatenate([lines[:, t * size : (t + 1) * size].T for t in range(planes)], axis=1)
    lines = jnp.concatenate(halves(lines), axis=1)
    tall, lanes = out_ref.shape[1:]
    taken = [jnp.zeros((tall, lanes), jnp.float32) for _ in range(2)]
    chip, core = chip_ref[0], core_ref[0]
    for m in range(bands):
        held, first, source, from_core = (mine_ref, 0, m, core) if m < chips else (theirs_ref, 2 * chips, m - chips, 1 - core)
        share = occupied_ref[2 * source + from_core].astype(jnp.float32) * (1.0 / coefs)
        weight_real = sums[:, first + source : first + source + 1] * share
        weight_imag = sums[:, first + chips + source : first + chips + source + 1] * share
        basis = held[lax.rem(chip + chips - source, chips)].reshape(2, tall, lanes)
        taken[0] = taken[0] + weight_real * basis[0] - weight_imag * basis[1]
        taken[1] = taken[1] + weight_imag * basis[0] + weight_real * basis[1]
    every_column = lax.broadcasted_iota(jnp.int32, (half, lanes), 0).astype(jnp.float32)
    for r in range(0, tall, 2):
        at_line = line_ref[:, r * lanes : (r + 2) * lanes]
        found = jnp.dot(lines, jnp.concatenate([at_line, at_line], axis=0), preferred_element_type=jnp.float32)
        for i in range(2):
            at_column = every_column == column_ref[r + i : r + i + 1, :]
            for p in range(2):
                applied = jnp.where(at_column, found[p * half : (p + 1) * half, i * lanes : (i + 1) * lanes], 0.0)
                out_ref[p, r + i : r + i + 1, :] = jnp.sum(applied, axis=0, keepdims=True) - taken[p][r + i : r + i + 1]


SCALARS = pl.BlockSpec(memory_space=pltpu.SMEM)
FAR = pl.BlockSpec(memory_space=pl.ANY)
WHOLE = pl.BlockSpec(memory_space=pltpu.VMEM)


def spread(owner, psi, points, table, size, owners):
    return pl.pallas_call(
        functools.partial(spread_kernel, size=size, owners=owners),
        out_shape=made((size * (size // (2 * owners)), size)),
        in_specs=[SCALARS, FAR, FAR, FAR],
        scratch_shapes=[
            pltpu.VMEM(psi.shape, psi.dtype),
            pltpu.VMEM(points.shape[1:], points.dtype),
            pltpu.VMEM(table.shape, table.dtype),
            pltpu.VMEM((6, *points.shape[1:]), jnp.float32),
            pltpu.SemaphoreType.DMA((3,)),
        ],
        interpret=INTERPRET,
        name="spread",
    )(owner, psi, points, table)


def fan(rows, copies):
    return pl.pallas_call(fan_kernel, out_shape=made((copies, *rows.shape)), interpret=INTERPRET, name="fan")(near(rows))


def carry(x, after):
    return pl.pallas_call(carry_kernel, out_shape=made(x.shape), in_specs=[WHOLE, FAR], interpret=INTERPRET, name="carry")(near(x), after)


def join(parts):
    return pl.pallas_call(join_kernel, out_shape=made((len(parts), *parts[0].shape)), interpret=INTERPRET, name="join")(*map(near, parts))


def sift(owner, points, after, size, owners):
    tall, lanes = points.shape[1:]
    return pl.pallas_call(
        functools.partial(sift_kernel, size=size, owners=owners),
        out_shape=(made((size // 2 * (size // (2 * owners)), tall * lanes), jnp.bfloat16), made((tall, lanes))),
        in_specs=[SCALARS, FAR, FAR],
        scratch_shapes=[pltpu.VMEM((tall, lanes), points.dtype), pltpu.VMEM((tall, lanes), jnp.float32), pltpu.SemaphoreType.DMA],
        interpret=INTERPRET,
        name="sift",
    )(owner, points, after)


def apply(field, potential, along_z, along_x, back_x, back_z, mine, size, owners):
    return pl.pallas_call(
        functools.partial(apply_kernel, size=size, owners=owners),
        out_shape=(made(field.shape), made((2 * mine.shape[0], size))),
        scratch_shapes=[pltpu.VMEM((2, *field.shape), jnp.float32)],
        interpret=INTERPRET,
        name="apply",
    )(*map(near, (field, potential, along_z, along_x, back_x, back_z, mine)))


def pair(theirs, product, sums, owners):
    return pl.pallas_call(
        functools.partial(pair_kernel, owners=owners),
        out_shape=made((product.shape[0] + owners, product.shape[1])),
        interpret=INTERPRET,
        name="pair",
    )(*map(near, (theirs, product, sums)))


def project(place, occupied, rows, picked, table, mine, theirs, size, owners, coefs):
    return pl.pallas_call(
        functools.partial(project_kernel, size=size, owners=owners, coefs=coefs),
        out_shape=jax.ShapeDtypeStruct((2, *picked[1].shape), jnp.float32),
        in_specs=[SCALARS, SCALARS, SCALARS] + [WHOLE] * 6,
        interpret=INTERPRET,
        name="project",
    )(*place, occupied, *map(near, (rows, *picked, table, mine, theirs)))


def along_ring(x, axis, step):
    count = lax.axis_size(axis)
    return lax.ppermute(x, axis, [(i, (i + step) % count) for i in range(count)])


def shards(psi, potential, miller, occupied):
    size = potential.shape[0]
    owners, chips = lax.axis_size("ga"), lax.axis_size("chip")
    block = psi.shape[2]
    along_y, along_z, along_x, back_x, back_z, back_y = tables(size, owners)
    owner, *place = (lax.axis_index(axis).reshape(1) for axis in ("ga", "chip", "core"))
    points = miller.reshape(-1, block // size, size)
    rows = spread(owner, psi.reshape(2, -1, size), points, along_y, size, owners)
    group = rows.shape[0] // owners
    rows = lax.all_to_all(rows.reshape(owners, group, size), "ga", split_axis=0, concat_axis=0, tiled=True)
    mine = lax.all_to_all(fan(rows, chips), "chip", split_axis=0, concat_axis=0, tiled=True)
    theirs = along_ring(mine, "core", 1)
    product, sums = apply(rows.reshape(-1, size), potential, along_z, along_x, back_x, back_z, mine, size, owners)
    sent = pair(theirs, product, sums, owners)
    rows = lax.all_to_all(sent.reshape(owners, 1, -1), "ga", split_axis=0, concat_axis=0, tiled=True).reshape(sent.shape)
    own = carry(psi.reshape(-1, size), sent)
    basis = join([own] + [along_ring(own, "chip", step) for step in range(1, chips)])
    other_basis = along_ring(basis, "core", 1)
    picked = sift(owner, points, sent, size, owners)
    out = project(place, occupied, rows, picked, back_y, basis, other_basis, size, owners, miller.shape[0])
    return out.reshape(2, 1, block)


def solution(mesh):
    groups, owners, bands = (mesh.shape[axis] for axis in ("pert", "ga", "band"))
    mesh = Mesh(mesh.devices.reshape(groups, owners, bands // 2, 2), ("pert", "ga", "chip", "core"))
    in_specs = (P(None, ("chip", "core"), "ga"), P("pert", "ga", None), P(), P())
    out_specs = P(None, ("pert", "chip", "core"), "ga")
    return jax.shard_map(shards, mesh=mesh, in_specs=in_specs, out_specs=out_specs, check_vma=False)
```

```python
import functools

import jax
import jax.numpy as jnp
import numpy as np
from jax import lax
from jax.experimental import pallas as pl
from jax.experimental.pallas import tpu as pltpu
from jax.sharding import Mesh
from jax.sharding import PartitionSpec as P

highest = lax.Precision.HIGHEST
INTERPRET = False


def near(x):
    return x if INTERPRET else pltpu.with_memory_space_constraint(x, pltpu.VMEM)


def made(shape, dtype=jnp.float32):
    return jax.ShapeDtypeStruct(shape, dtype) if INTERPRET else pltpu.VMEM(shape, dtype)


def halves(x):
    high = x.astype(jnp.bfloat16)
    return high, (x - high.astype(jnp.float32)).astype(jnp.bfloat16)


def dot(a, b):
    part = functools.partial(jnp.dot, preferred_element_type=jnp.float32)
    return part(a[0], b[0]) + (part(a[0], b[1]) + part(a[1], b[0]))


def turned(x):
    half = x.shape[1] // 2
    return jnp.concatenate([-x[:, half:], x[:, :half]], axis=1)


def ring(owners):
    return [(i + owners // 2) % owners for i in range(owners)]


def tables(size, owners):
    order = np.asarray(ring(owners))
    signed = np.arange(size // 2) - size // 4
    angle = 2.0 * np.pi / size * (np.arange(size)[:, None] * signed[None, :] % size)
    cosine, sine = np.cos(angle), np.sin(angle)
    by_owner = [part.reshape(owners, size // owners, -1)[order] for part in (cosine, sine)]
    along_y = np.concatenate([part.reshape(size, -1) for part in by_owner], axis=1)
    along_z = np.block([[cosine.T, sine.T], [-sine.T, cosine.T]])
    planes = [part.reshape(size, -1, owners)[:, :, order].reshape(size, -1) for part in (cosine, sine)]
    along_x = np.block([[planes[0], -planes[1]], [planes[1], planes[0]]])
    back = [part.transpose(2, 1, 0).reshape(size // 2, size) for part in by_owner]
    back_y = np.concatenate([back[0], -back[1]], axis=1)

    def both(table):
        table = np.asarray(table, np.float32)
        high = table.astype(jnp.bfloat16)
        return np.stack([high, (table - high.astype(np.float32)).astype(jnp.bfloat16)])

    return tuple(map(both, (along_y, along_z, along_x, along_x.T, along_z.T / size**3, back_y)))


def places(points, size, owners):
    quarter = size // 4
    plane = (points // (size * size) + quarter) % size
    row = (points // size + quarter) % size
    column = (points + quarter) % size
    return plane // owners * (size // 2) + row, column


def own_points(owner_ref, points_ref, held_ref, sem):
    return pltpu.make_async_copy(points_ref.at[owner_ref[0]], held_ref, sem)


def numbered(count, lanes):
    return lax.broadcasted_iota(jnp.int32, (count, lanes), 0).astype(jnp.float32).astype(jnp.bfloat16)


def copied_down(row, count):
    some = jnp.broadcast_to(row, (16, row.shape[1])).astype(jnp.bfloat16)
    return jnp.concatenate([some] * (count // 16), axis=0)


def spread_kernel(
    owner_ref, core_ref, psi_ref, points_ref, along_ref, out_ref, psi_held, points_held, along_held, flat_ref, sems, *, size, owners
):
    del core_ref
    copies = [
        own_points(owner_ref, points_ref, points_held, sems.at[0]),
        pltpu.make_async_copy(psi_ref, psi_held, sems.at[1]),
        pltpu.make_async_copy(along_ref, along_held, sems.at[2]),
    ]
    for copy in copies:
        copy.start()
    half = size // 2
    lines = half * half // owners
    copies[0].wait()
    line, column = places(points_held[...], size, owners)
    flat_ref[0], flat_ref[1] = line.astype(jnp.float32), column.astype(jnp.float32)
    copies[1].wait()
    for part in range(2):
        for which, x in enumerate(halves(psi_held[part])):
            flat_ref[2 + 2 * which + part] = x.astype(jnp.float32)
    tall, lanes = points_held.shape
    every_line, every_column = numbered(lines, lanes), numbered(half, lanes)
    one, zero = jnp.ones((), jnp.bfloat16), jnp.zeros((), jnp.bfloat16)
    at_line, values = [], []
    for r in range(tall):
        at_line.append(jnp.where(every_line == copied_down(flat_ref[0, r : r + 1, :], lines), one, zero))
        at_column = every_column == copied_down(flat_ref[1, r : r + 1, :], half)
        parts = [jnp.where(at_column, copied_down(flat_ref[i, r : r + 1, :], half), zero) for i in range(2, 6)]
        values.append(jnp.concatenate(parts, axis=0))
    at_line, values = jnp.concatenate(at_line, axis=1), jnp.concatenate(values, axis=1)
    total = lax.dot_general(at_line, values, (((1,), (1,)), ((), ())), preferred_element_type=jnp.float32)
    total = total[:, :size] + total[:, size:]
    around = turned(total)
    planes = lines // half
    fields = [jnp.concatenate([x[t * half : (t + 1) * half] for x in (total, around)], axis=0) for t in range(planes)]
    copies[2].wait()
    rows = dot(along_held[...], halves(jnp.concatenate(fields, axis=1)))
    for t in range(planes):
        out_ref[pl.ds(t, size, stride=planes), :] = rows[:, t * size : (t + 1) * size]


def fan_kernel(rows_ref, psi_ref, out_ref):
    for i in range(out_ref.shape[0]):
        out_ref[i, : rows_ref.shape[0]] = rows_ref[...]
        out_ref[i, rows_ref.shape[0] :] = psi_ref[...]


def apply_kernel(field_ref, potential_ref, z_ref, x_ref, back_x_ref, back_z_ref, mine_ref, out_ref, sums_ref, wide_ref, *, size, owners):
    per, own = size // (2 * owners), size // owners
    group = per * own
    wide = dot(halves(field_ref[...]), z_ref[...])
    for part in range(2):
        wide_ref[part] = wide[:, part * size : (part + 1) * size]

    def planes(y, part):
        return [wide_ref[part, pl.ds(y * per + t, owners, stride=group), :] for t in range(per)]

    columns = [jnp.concatenate(planes(y, 0) + planes(y, 1), axis=0) for y in range(own)]
    wave = dot(x_ref[...], halves(jnp.concatenate(columns, axis=1)))
    scale = jnp.concatenate([potential_ref[:, y, :] for y in range(own)], axis=1)
    product = jnp.concatenate([wave[:size] * scale, wave[size:] * scale], axis=0)
    back = dot(back_x_ref[...], halves(product))
    for y in range(own):
        for t in range(per):
            for part in range(2):
                first = (part * per + t) * owners
                wide_ref[part, pl.ds(y * per + t, owners, stride=group), :] = back[first : first + owners, y * size : (y + 1) * size]
    product = dot(halves(jnp.concatenate([wide_ref[0], wide_ref[1]], axis=1)), back_z_ref[...])
    out_ref[...] = product
    sums_ref[...] = overlaps(mine_ref, product, owners)


def overlaps(fields_ref, product, owners):
    half = product.shape[1] // 2
    crossed = jnp.concatenate([product[:, half:], -product[:, :half]], axis=1)
    fields = [fields_ref[m, :owners].reshape(product.shape) for m in range(fields_ref.shape[0])]
    return jnp.concatenate([jnp.sum(f * other, axis=0, keepdims=True) for other in (product, crossed) for f in fields], axis=0)


def pair_kernel(theirs_ref, product_ref, sums_ref, out_ref, *, owners):
    lanes = product_ref.shape[1]
    group = product_ref.shape[0] // owners
    sums = jnp.concatenate([sums_ref[...], overlaps(theirs_ref, product_ref[...], owners)], axis=0)
    sums = jnp.dot(sums, jnp.ones((lanes, lanes), jnp.float32), precision=highest, preferred_element_type=jnp.float32)
    on_diagonal = lax.broadcasted_iota(jnp.int32, sums.shape, 0) == lax.broadcasted_iota(jnp.int32, sums.shape, 1)
    row = jnp.sum(jnp.where(on_diagonal, sums, 0.0), axis=0, keepdims=True)
    for r in range(group):
        out_ref[pl.ds(r, owners, stride=group + 1), :] = product_ref[pl.ds(r, owners, stride=group), :]
    out_ref[pl.ds(group, owners, stride=group + 1), :] = jnp.broadcast_to(row, (owners, lanes))


def project_kernel(
    owner_ref, core_ref, occupied_ref, rows_ref, points_ref, along_ref, mine_ref, theirs_ref, out_ref, held_ref, flat_ref, sem, *, size, owners, coefs
):
    copy = own_points(owner_ref, points_ref, held_ref, sem)
    copy.start()
    chips = mine_ref.shape[0]
    bands = 2 * chips
    half = size // 2
    group = rows_ref.shape[0] // owners
    planes = half // owners
    sums = jnp.sum(rows_ref[pl.ds(group - 1, owners, stride=group), :], axis=0, keepdims=True)
    fields = []
    for t in range(planes):
        rows = [rows_ref[pl.ds(r, owners, stride=group), :] for r in range(t, group - 1, planes)]
        rows = jnp.concatenate(rows, axis=0)
        fields.append(jnp.concatenate([rows, turned(rows)], axis=0))
    lines = dot(along_ref[...], halves(jnp.concatenate(fields, axis=1)))
    lines = jnp.concatenate([lines[:, t * size : (t + 1) * size].T for t in range(planes)], axis=1)
    lines = jnp.concatenate(halves(lines), axis=1)
    copy.wait()
    line, column = places(held_ref[...], size, owners)
    flat_ref[0], flat_ref[1] = line.astype(jnp.float32), column.astype(jnp.float32)
    tall, lanes = out_ref.shape[1:]
    taken = [jnp.zeros((tall, lanes), jnp.float32) for _ in range(2)]
    core = core_ref[0]
    for m in range(bands):
        held, first, source, from_core = (mine_ref, 0, m, core) if m < chips else (theirs_ref, 2 * chips, m - chips, 1 - core)
        share = occupied_ref[2 * source + from_core].astype(jnp.float32) * (1.0 / coefs)
        weight_real = sums[:, first + source : first + source + 1] * share
        weight_imag = sums[:, first + chips + source : first + chips + source + 1] * share
        basis = held[source, owners:].reshape(2, tall, lanes)
        taken[0] = taken[0] + weight_real * basis[0] - weight_imag * basis[1]
        taken[1] = taken[1] + weight_imag * basis[0] + weight_real * basis[1]
    every_line = numbered(planes * half, lanes)
    every_column = lax.broadcasted_iota(jnp.int32, (half, lanes), 0).astype(jnp.float32)
    one, zero = jnp.ones((), jnp.bfloat16), jnp.zeros((), jnp.bfloat16)
    for r in range(0, tall, 2):
        at_line = [jnp.where(every_line == copied_down(flat_ref[0, i : i + 1, :], planes * half), one, zero) for i in (r, r + 1)]
        at_line = jnp.concatenate(at_line, axis=1)
        found = jnp.dot(lines, jnp.concatenate([at_line, at_line], axis=0), preferred_element_type=jnp.float32)
        for i in range(2):
            at_column = every_column == flat_ref[1, r + i : r + i + 1, :]
            for p in range(2):
                applied = jnp.where(at_column, found[p * half : (p + 1) * half, i * lanes : (i + 1) * lanes], 0.0)
                out_ref[p, r + i : r + i + 1, :] = jnp.sum(applied, axis=0, keepdims=True) - taken[p][r + i : r + i + 1]


SCALARS = pl.BlockSpec(memory_space=pltpu.SMEM)
FAR = pl.BlockSpec(memory_space=pl.ANY)
WHOLE = pl.BlockSpec(memory_space=pltpu.VMEM)


def spread(owner, core, psi, points, table, size, owners):
    return pl.pallas_call(
        functools.partial(spread_kernel, size=size, owners=owners),
        out_shape=made((size * (size // (2 * owners)), size)),
        in_specs=[SCALARS, SCALARS, FAR, FAR, FAR],
        scratch_shapes=[
            pltpu.VMEM(psi.shape, psi.dtype),
            pltpu.VMEM(points.shape[1:], points.dtype),
            pltpu.VMEM(table.shape, table.dtype),
            pltpu.VMEM((6, *points.shape[1:]), jnp.float32),
            pltpu.SemaphoreType.DMA((3,)),
        ],
        interpret=INTERPRET,
        name="spread",
    )(owner, core, psi, points, table)


def fan(rows, psi, copies):
    shape = (copies, rows.shape[0] + psi.shape[0], *rows.shape[1:])
    return pl.pallas_call(fan_kernel, out_shape=made(shape), interpret=INTERPRET, name="fan")(near(rows), near(psi))


def apply(field, potential, along_z, along_x, back_x, back_z, mine, size, owners):
    return pl.pallas_call(
        functools.partial(apply_kernel, size=size, owners=owners),
        out_shape=(made(field.shape), made((2 * mine.shape[0], size))),
        scratch_shapes=[pltpu.VMEM((2, *field.shape), jnp.float32)],
        interpret=INTERPRET,
        name="apply",
    )(*map(near, (field, potential, along_z, along_x, back_x, back_z, mine)))


def pair(theirs, product, sums, owners):
    return pl.pallas_call(
        functools.partial(pair_kernel, owners=owners),
        out_shape=made((product.shape[0] + owners, product.shape[1])),
        interpret=INTERPRET,
        name="pair",
    )(*map(near, (theirs, product, sums)))


def project(owner, core, occupied, rows, points, table, mine, theirs, size, owners, coefs):
    tall, lanes = points.shape[1:]
    return pl.pallas_call(
        functools.partial(project_kernel, size=size, owners=owners, coefs=coefs),
        out_shape=jax.ShapeDtypeStruct((2, tall, lanes), jnp.float32),
        in_specs=[SCALARS, SCALARS, SCALARS, WHOLE, FAR, WHOLE, WHOLE, WHOLE],
        scratch_shapes=[pltpu.VMEM((tall, lanes), points.dtype), pltpu.VMEM((2, tall, lanes), jnp.float32), pltpu.SemaphoreType.DMA],
        interpret=INTERPRET,
        name="project",
    )(owner, core, occupied, near(rows), points, near(table), near(mine), near(theirs))


def exchanged(x, axis):
    groups = [ring(lax.axis_size(axis))]
    return lax.all_to_all(x, axis, split_axis=0, concat_axis=0, axis_index_groups=groups, tiled=True)


def along_ring(x, axis, step):
    count = lax.axis_size(axis)
    return lax.ppermute(x, axis, [(i, (i + step) % count) for i in range(count)])


def shards(psi, potential, miller, occupied):
    size = potential.shape[0]
    owners, chips = lax.axis_size("ga"), lax.axis_size("chip")
    block = psi.shape[2]
    along_y, along_z, along_x, back_x, back_z, back_y = tables(size, owners)
    owner, core = (lax.axis_index(axis).reshape(1) for axis in ("ga", "core"))
    points = miller.reshape(-1, block // size, size)
    rows = spread(owner, core, psi.reshape(2, -1, size), points, along_y, size, owners)
    group = rows.shape[0] // owners
    rows = exchanged(rows.reshape(owners, group, size), "ga")
    sent = fan(rows, psi.reshape(-1, group, size), chips)
    mine = lax.all_to_all(sent, "chip", split_axis=0, concat_axis=0, tiled=True)
    theirs = along_ring(mine, "core", 1)
    product, sums = apply(rows.reshape(-1, size), potential, along_z, along_x, back_x, back_z, mine, size, owners)
    sent = pair(theirs, product, sums, owners)
    rows = exchanged(sent.reshape(owners, 1, -1), "ga").reshape(sent.shape)
    out = project(owner, core, occupied, rows, points, back_y, mine, theirs, size, owners, miller.shape[0])
    return out.reshape(2, 1, block)


def solution(mesh):
    groups, owners, bands = (mesh.shape[axis] for axis in ("pert", "ga", "band"))
    mesh = Mesh(mesh.devices.reshape(groups, owners, bands // 2, 2), ("pert", "ga", "chip", "core"))
    in_specs = (P(None, ("chip", "core"), "ga"), P("pert", "ga", None), P(), P())
    out_specs = P(None, ("pert", "chip", "core"), "ga")
    return jax.shard_map(shards, mesh=mesh, in_specs=in_specs, out_specs=out_specs, check_vma=False)
```

```python
import functools

import jax
import jax.numpy as jnp
import numpy as np
from jax import lax
from jax.experimental import pallas as pl
from jax.experimental.pallas import tpu as pltpu
from jax.sharding import Mesh
from jax.sharding import PartitionSpec as P

highest = lax.Precision.HIGHEST
INTERPRET = False


def near(x):
    return x if INTERPRET else pltpu.with_memory_space_constraint(x, pltpu.VMEM)


def made(shape, dtype=jnp.float32):
    return jax.ShapeDtypeStruct(shape, dtype) if INTERPRET else pltpu.VMEM(shape, dtype)


def halves(x):
    high = x.astype(jnp.bfloat16)
    return high, (x - high.astype(jnp.float32)).astype(jnp.bfloat16)


def dot(a, b):
    part = functools.partial(jnp.dot, preferred_element_type=jnp.float32)
    return part(a[0], b[0]) + (part(a[0], b[1]) + part(a[1], b[0]))


def turned(x):
    half = x.shape[1] // 2
    return jnp.concatenate([-x[:, half:], x[:, :half]], axis=1)


def listed(count, first):
    return [(first + i) % count for i in range(count)]


def ring(owners):
    return listed(owners, owners - 1)


def row(chips):
    return listed(chips, chips // 2)


def tables(size, owners):
    order = np.asarray(ring(owners))
    signed = np.arange(size // 2) - size // 4
    angle = 2.0 * np.pi / size * (np.arange(size)[:, None] * signed[None, :] % size)
    cosine, sine = np.cos(angle), np.sin(angle)
    by_owner = [part.reshape(owners, size // owners, -1)[order] for part in (cosine, sine)]
    along_y = np.concatenate([part.reshape(size, -1) for part in by_owner], axis=1)
    along_z = np.block([[cosine.T, sine.T], [-sine.T, cosine.T]])
    planes = [part.reshape(size, -1, owners)[:, :, order].reshape(size, -1) for part in (cosine, sine)]
    along_x = np.block([[planes[0], -planes[1]], [planes[1], planes[0]]])
    back = [part.transpose(2, 1, 0).reshape(size // 2, size) for part in by_owner]
    back_y = np.concatenate([back[0], -back[1]], axis=1)

    def both(table):
        table = np.asarray(table, np.float32)
        high = table.astype(jnp.bfloat16)
        return np.stack([high, (table - high.astype(np.float32)).astype(jnp.bfloat16)])

    return tuple(map(both, (along_y, along_z, along_x, along_x.T, along_z.T / size**3, back_y)))


def places(points, size, owners):
    quarter = size // 4
    plane = (points // (size * size) + quarter) % size
    row = (points // size + quarter) % size
    column = (points + quarter) % size
    return plane // owners * (size // 2) + row, column


def own_points(owner_ref, points_ref, held_ref, sem):
    return pltpu.make_async_copy(points_ref.at[owner_ref[0]], held_ref, sem)


def numbered(count, lanes):
    return lax.broadcasted_iota(jnp.int32, (count, lanes), 0).astype(jnp.float32).astype(jnp.bfloat16)


def copied_down(row, count):
    some = jnp.broadcast_to(row, (16, row.shape[1])).astype(jnp.bfloat16)
    return jnp.concatenate([some] * (count // 16), axis=0)


def spread_kernel(
    owner_ref, core_ref, psi_ref, points_ref, along_ref, out_ref, psi_held, points_held, along_held, flat_ref, sems, *, size, owners
):
    del core_ref
    copies = [
        own_points(owner_ref, points_ref, points_held, sems.at[0]),
        pltpu.make_async_copy(psi_ref, psi_held, sems.at[1]),
        pltpu.make_async_copy(along_ref, along_held, sems.at[2]),
    ]
    for copy in copies:
        copy.start()
    half = size // 2
    lines = half * half // owners
    copies[0].wait()
    line, column = places(points_held[...], size, owners)
    flat_ref[0], flat_ref[1] = line.astype(jnp.float32), column.astype(jnp.float32)
    copies[1].wait()
    for part in range(2):
        for which, x in enumerate(halves(psi_held[part])):
            flat_ref[2 + 2 * which + part] = x.astype(jnp.float32)
    tall, lanes = points_held.shape
    every_line, every_column = numbered(lines, lanes), numbered(half, lanes)
    one, zero = jnp.ones((), jnp.bfloat16), jnp.zeros((), jnp.bfloat16)
    at_line, values = [], []
    for r in range(tall):
        at_line.append(jnp.where(every_line == copied_down(flat_ref[0, r : r + 1, :], lines), one, zero))
        at_column = every_column == copied_down(flat_ref[1, r : r + 1, :], half)
        parts = [jnp.where(at_column, copied_down(flat_ref[i, r : r + 1, :], half), zero) for i in range(2, 6)]
        values.append(jnp.concatenate(parts, axis=0))
    at_line, values = jnp.concatenate(at_line, axis=1), jnp.concatenate(values, axis=1)
    total = lax.dot_general(at_line, values, (((1,), (1,)), ((), ())), preferred_element_type=jnp.float32)
    total = total[:, :size] + total[:, size:]
    around = turned(total)
    planes = lines // half
    fields = [jnp.concatenate([x[t * half : (t + 1) * half] for x in (total, around)], axis=0) for t in range(planes)]
    copies[2].wait()
    rows = dot(along_held[...], halves(jnp.concatenate(fields, axis=1)))
    for t in range(planes):
        out_ref[pl.ds(t, size, stride=planes), :] = rows[:, t * size : (t + 1) * size]


def fan_kernel(rows_ref, psi_ref, out_ref):
    for i in range(out_ref.shape[0]):
        out_ref[i, : rows_ref.shape[0]] = rows_ref[...]
        out_ref[i, rows_ref.shape[0] :] = psi_ref[...]


def apply_kernel(field_ref, potential_ref, z_ref, x_ref, back_x_ref, back_z_ref, mine_ref, out_ref, sums_ref, wide_ref, *, size, owners):
    per, own = size // (2 * owners), size // owners
    group = per * own
    wide = dot(halves(field_ref[...]), z_ref[...])
    for part in range(2):
        wide_ref[part] = wide[:, part * size : (part + 1) * size]

    def planes(y, part):
        return [wide_ref[part, pl.ds(y * per + t, owners, stride=group), :] for t in range(per)]

    columns = [jnp.concatenate(planes(y, 0) + planes(y, 1), axis=0) for y in range(own)]
    wave = dot(x_ref[...], halves(jnp.concatenate(columns, axis=1)))
    scale = jnp.concatenate([potential_ref[:, y, :] for y in range(own)], axis=1)
    product = jnp.concatenate([wave[:size] * scale, wave[size:] * scale], axis=0)
    back = dot(back_x_ref[...], halves(product))
    for y in range(own):
        for t in range(per):
            for part in range(2):
                first = (part * per + t) * owners
                wide_ref[part, pl.ds(y * per + t, owners, stride=group), :] = back[first : first + owners, y * size : (y + 1) * size]
    product = dot(halves(jnp.concatenate([wide_ref[0], wide_ref[1]], axis=1)), back_z_ref[...])
    out_ref[...] = product
    sums_ref[...] = overlaps(mine_ref, product, owners)


def overlaps(fields_ref, product, owners):
    half = product.shape[1] // 2
    crossed = jnp.concatenate([product[:, half:], -product[:, :half]], axis=1)
    fields = [fields_ref[m, :owners].reshape(product.shape) for m in range(fields_ref.shape[0])]
    return jnp.concatenate([jnp.sum(f * other, axis=0, keepdims=True) for other in (product, crossed) for f in fields], axis=0)


def pair_kernel(theirs_ref, product_ref, sums_ref, out_ref, *, owners):
    lanes = product_ref.shape[1]
    group = product_ref.shape[0] // owners
    sums = jnp.concatenate([sums_ref[...], overlaps(theirs_ref, product_ref[...], owners)], axis=0)
    sums = jnp.dot(sums, jnp.ones((lanes, lanes), jnp.float32), precision=highest, preferred_element_type=jnp.float32)
    on_diagonal = lax.broadcasted_iota(jnp.int32, sums.shape, 0) == lax.broadcasted_iota(jnp.int32, sums.shape, 1)
    row = jnp.sum(jnp.where(on_diagonal, sums, 0.0), axis=0, keepdims=True)
    for r in range(group):
        out_ref[pl.ds(r, owners, stride=group + 1), :] = product_ref[pl.ds(r, owners, stride=group), :]
    out_ref[pl.ds(group, owners, stride=group + 1), :] = jnp.broadcast_to(row, (owners, lanes))


def project_kernel(
    owner_ref, core_ref, occupied_ref, rows_ref, points_ref, along_ref, mine_ref, theirs_ref, out_ref, held_ref, flat_ref, sem, *, size, owners, coefs
):
    copy = own_points(owner_ref, points_ref, held_ref, sem)
    copy.start()
    chips = mine_ref.shape[0]
    bands = 2 * chips
    half = size // 2
    group = rows_ref.shape[0] // owners
    planes = half // owners
    sums = jnp.sum(rows_ref[pl.ds(group - 1, owners, stride=group), :], axis=0, keepdims=True)
    fields = []
    for t in range(planes):
        rows = [rows_ref[pl.ds(r, owners, stride=group), :] for r in range(t, group - 1, planes)]
        rows = jnp.concatenate(rows, axis=0)
        fields.append(jnp.concatenate([rows, turned(rows)], axis=0))
    lines = dot(along_ref[...], halves(jnp.concatenate(fields, axis=1)))
    lines = jnp.concatenate([lines[:, t * size : (t + 1) * size].T for t in range(planes)], axis=1)
    lines = jnp.concatenate(halves(lines), axis=1)
    copy.wait()
    line, column = places(held_ref[...], size, owners)
    flat_ref[0], flat_ref[1] = line.astype(jnp.float32), column.astype(jnp.float32)
    tall, lanes = out_ref.shape[1:]
    taken = [jnp.zeros((tall, lanes), jnp.float32) for _ in range(2)]
    core = core_ref[0]
    for m in range(bands):
        held, first, source, from_core = (mine_ref, 0, m, core) if m < chips else (theirs_ref, 2 * chips, m - chips, 1 - core)
        share = occupied_ref[2 * row(chips)[source] + from_core].astype(jnp.float32) * (1.0 / coefs)
        weight_real = sums[:, first + source : first + source + 1] * share
        weight_imag = sums[:, first + chips + source : first + chips + source + 1] * share
        basis = held[source, owners:].reshape(2, tall, lanes)
        taken[0] = taken[0] + weight_real * basis[0] - weight_imag * basis[1]
        taken[1] = taken[1] + weight_imag * basis[0] + weight_real * basis[1]
    every_line = numbered(planes * half, lanes)
    every_column = lax.broadcasted_iota(jnp.int32, (half, lanes), 0).astype(jnp.float32)
    one, zero = jnp.ones((), jnp.bfloat16), jnp.zeros((), jnp.bfloat16)
    for r in range(0, tall, 2):
        at_line = [jnp.where(every_line == copied_down(flat_ref[0, i : i + 1, :], planes * half), one, zero) for i in (r, r + 1)]
        at_line = jnp.concatenate(at_line, axis=1)
        found = jnp.dot(lines, jnp.concatenate([at_line, at_line], axis=0), preferred_element_type=jnp.float32)
        for i in range(2):
            at_column = every_column == flat_ref[1, r + i : r + i + 1, :]
            for p in range(2):
                applied = jnp.where(at_column, found[p * half : (p + 1) * half, i * lanes : (i + 1) * lanes], 0.0)
                out_ref[p, r + i : r + i + 1, :] = jnp.sum(applied, axis=0, keepdims=True) - taken[p][r + i : r + i + 1]


SCALARS = pl.BlockSpec(memory_space=pltpu.SMEM)
FAR = pl.BlockSpec(memory_space=pl.ANY)
WHOLE = pl.BlockSpec(memory_space=pltpu.VMEM)


def spread(owner, core, psi, points, table, size, owners):
    return pl.pallas_call(
        functools.partial(spread_kernel, size=size, owners=owners),
        out_shape=made((size * (size // (2 * owners)), size)),
        in_specs=[SCALARS, SCALARS, FAR, FAR, FAR],
        scratch_shapes=[
            pltpu.VMEM(psi.shape, psi.dtype),
            pltpu.VMEM(points.shape[1:], points.dtype),
            pltpu.VMEM(table.shape, table.dtype),
            pltpu.VMEM((6, *points.shape[1:]), jnp.float32),
            pltpu.SemaphoreType.DMA((3,)),
        ],
        interpret=INTERPRET,
        name="spread",
    )(owner, core, psi, points, table)


def fan(rows, psi, copies):
    shape = (copies, rows.shape[0] + psi.shape[0], *rows.shape[1:])
    return pl.pallas_call(fan_kernel, out_shape=made(shape), interpret=INTERPRET, name="fan")(near(rows), near(psi))


def apply(field, potential, along_z, along_x, back_x, back_z, mine, size, owners):
    return pl.pallas_call(
        functools.partial(apply_kernel, size=size, owners=owners),
        out_shape=(made(field.shape), made((2 * mine.shape[0], size))),
        scratch_shapes=[pltpu.VMEM((2, *field.shape), jnp.float32)],
        interpret=INTERPRET,
        name="apply",
    )(*map(near, (field, potential, along_z, along_x, back_x, back_z, mine)))


def pair(theirs, product, sums, owners):
    return pl.pallas_call(
        functools.partial(pair_kernel, owners=owners),
        out_shape=made((product.shape[0] + owners, product.shape[1])),
        interpret=INTERPRET,
        name="pair",
    )(*map(near, (theirs, product, sums)))


def project(owner, core, occupied, rows, points, table, mine, theirs, size, owners, coefs):
    tall, lanes = points.shape[1:]
    return pl.pallas_call(
        functools.partial(project_kernel, size=size, owners=owners, coefs=coefs),
        out_shape=jax.ShapeDtypeStruct((2, tall, lanes), jnp.float32),
        in_specs=[SCALARS, SCALARS, SCALARS, WHOLE, FAR, WHOLE, WHOLE, WHOLE],
        scratch_shapes=[pltpu.VMEM((tall, lanes), points.dtype), pltpu.VMEM((2, tall, lanes), jnp.float32), pltpu.SemaphoreType.DMA],
        interpret=INTERPRET,
        name="project",
    )(owner, core, occupied, near(rows), points, near(table), near(mine), near(theirs))


def exchanged(x, axis, order):
    return lax.all_to_all(x, axis, split_axis=0, concat_axis=0, axis_index_groups=[order], tiled=True)


def along_ring(x, axis, step):
    count = lax.axis_size(axis)
    return lax.ppermute(x, axis, [(i, (i + step) % count) for i in range(count)])


def shards(psi, potential, miller, occupied):
    size = potential.shape[0]
    owners, chips = lax.axis_size("ga"), lax.axis_size("chip")
    block = psi.shape[2]
    along_y, along_z, along_x, back_x, back_z, back_y = tables(size, owners)
    owner, core = (lax.axis_index(axis).reshape(1) for axis in ("ga", "core"))
    points = miller.reshape(-1, block // size, size)
    rows = spread(owner, core, psi.reshape(2, -1, size), points, along_y, size, owners)
    group = rows.shape[0] // owners
    rows = exchanged(rows.reshape(owners, group, size), "ga", ring(owners))
    sent = fan(rows, psi.reshape(-1, group, size), chips)
    mine = exchanged(sent, "chip", row(chips))
    theirs = along_ring(mine, "core", 1)
    product, sums = apply(rows.reshape(-1, size), potential, along_z, along_x, back_x, back_z, mine, size, owners)
    sent = pair(theirs, product, sums, owners)
    rows = exchanged(sent.reshape(owners, 1, -1), "ga", ring(owners)).reshape(sent.shape)
    out = project(owner, core, occupied, rows, points, back_y, mine, theirs, size, owners, miller.shape[0])
    return out.reshape(2, 1, block)


def solution(mesh):
    groups, owners, bands = (mesh.shape[axis] for axis in ("pert", "ga", "band"))
    mesh = Mesh(mesh.devices.reshape(groups, owners, bands // 2, 2), ("pert", "ga", "chip", "core"))
    in_specs = (P(None, ("chip", "core"), "ga"), P("pert", "ga", None), P(), P())
    out_specs = P(None, ("pert", "chip", "core"), "ga")
    return jax.shard_map(shards, mesh=mesh, in_specs=in_specs, out_specs=out_specs, check_vma=False)
```

```python
import functools

import jax
import jax.numpy as jnp
import numpy as np
from jax import lax
from jax.experimental import pallas as pl
from jax.experimental.pallas import tpu as pltpu
from jax.sharding import Mesh
from jax.sharding import PartitionSpec as P

highest = lax.Precision.HIGHEST
INTERPRET = False


def near(x):
    return x if INTERPRET else pltpu.with_memory_space_constraint(x, pltpu.VMEM)


def made(shape, dtype=jnp.float32):
    return jax.ShapeDtypeStruct(shape, dtype) if INTERPRET else pltpu.VMEM(shape, dtype)


def halves(x):
    high = x.astype(jnp.bfloat16)
    return high, (x - high.astype(jnp.float32)).astype(jnp.bfloat16)


def dot(a, b):
    part = functools.partial(jnp.dot, preferred_element_type=jnp.float32)
    return part(a[0], b[0]) + (part(a[0], b[1]) + part(a[1], b[0]))


def turned(x):
    half = x.shape[1] // 2
    return jnp.concatenate([-x[:, half:], x[:, :half]], axis=1)


def listed(count, first):
    return [(first + i) % count for i in range(count)]


def ring(owners):
    return listed(owners, owners - 1)


def row(chips):
    return listed(chips, chips // 2)


def tables(size, owners):
    order = np.asarray(ring(owners))
    signed = np.arange(size // 2) - size // 4
    angle = 2.0 * np.pi / size * (np.arange(size)[:, None] * signed[None, :] % size)
    cosine, sine = np.cos(angle), np.sin(angle)
    by_owner = [part.reshape(owners, size // owners, -1)[order] for part in (cosine, sine)]
    along_y = np.concatenate([part.reshape(size, -1) for part in by_owner], axis=1)
    along_z = np.block([[cosine.T, sine.T], [-sine.T, cosine.T]])
    planes = [part.reshape(size, -1, owners)[:, :, order].reshape(size, -1) for part in (cosine, sine)]
    along_x = np.block([[planes[0], -planes[1]], [planes[1], planes[0]]])
    back = [part.transpose(2, 1, 0).reshape(size // 2, size) for part in by_owner]
    back_y = np.concatenate(back, axis=0)

    def both(table):
        table = np.asarray(table, np.float32)
        high = table.astype(jnp.bfloat16)
        return np.stack([high, (table - high.astype(np.float32)).astype(jnp.bfloat16)])

    return tuple(map(both, (along_y, along_z, along_x, along_x.T, along_z.T / size**3, back_y)))


def places(points, size, owners):
    quarter = size // 4
    plane = (points // (size * size) + quarter) % size
    row = (points // size + quarter) % size
    column = (points + quarter) % size
    return plane // owners * (size // 2) + row, column


def own_points(owner_ref, points_ref, held_ref, sem):
    return pltpu.make_async_copy(points_ref.at[owner_ref[0]], held_ref, sem)


def numbered(count, lanes):
    return lax.broadcasted_iota(jnp.int32, (count, lanes), 0).astype(jnp.float32).astype(jnp.bfloat16)


def copied_down(row, count):
    some = jnp.broadcast_to(row, (16, row.shape[1])).astype(jnp.bfloat16)
    return jnp.concatenate([some] * (count // 16), axis=0)


def spread_kernel(
    owner_ref, core_ref, psi_ref, points_ref, along_ref, out_ref, at_ref, psi_held, points_held, along_held, flat_ref, sems, *, size, owners
):
    del core_ref
    copies = [
        own_points(owner_ref, points_ref, points_held, sems.at[0]),
        pltpu.make_async_copy(psi_ref, psi_held, sems.at[1]),
        pltpu.make_async_copy(along_ref, along_held, sems.at[2]),
    ]
    for copy in copies:
        copy.start()
    half = size // 2
    lines = half * half // owners
    copies[0].wait()
    for i, x in enumerate(places(points_held[...], size, owners)):
        at_ref[i] = x.astype(jnp.float32)
    copies[1].wait()
    for part in range(2):
        for which, x in enumerate(halves(psi_held[part])):
            flat_ref[2 * which + part] = x.astype(jnp.float32)
    tall, lanes = points_held.shape
    every_line, every_column = numbered(lines, lanes), numbered(half, lanes)
    one, zero = jnp.ones((), jnp.bfloat16), jnp.zeros((), jnp.bfloat16)
    at_line, values = [], []
    for r in range(tall):
        at_line.append(jnp.where(every_line == copied_down(at_ref[0, r : r + 1, :], lines), one, zero))
        at_column = every_column == copied_down(at_ref[1, r : r + 1, :], half)
        parts = [jnp.where(at_column, copied_down(flat_ref[i, r : r + 1, :], half), zero) for i in range(4)]
        values.append(jnp.concatenate(parts, axis=0))
    at_line, values = jnp.concatenate(at_line, axis=1), jnp.concatenate(values, axis=1)
    total = lax.dot_general(at_line, values, (((1,), (1,)), ((), ())), preferred_element_type=jnp.float32)
    total = total[:, :size] + total[:, size:]
    around = turned(total)
    planes = lines // half
    fields = [jnp.concatenate([x[t * half : (t + 1) * half] for x in (total, around)], axis=0) for t in range(planes)]
    copies[2].wait()
    rows = dot(along_held[...], halves(jnp.concatenate(fields, axis=1)))
    for t in range(planes):
        out_ref[pl.ds(t, size, stride=planes), :] = rows[:, t * size : (t + 1) * size]


def fan_kernel(rows_ref, psi_ref, out_ref):
    for i in range(out_ref.shape[0]):
        out_ref[i, : rows_ref.shape[0]] = rows_ref[...]
        out_ref[i, rows_ref.shape[0] :] = psi_ref[...]


def apply_kernel(field_ref, potential_ref, z_ref, x_ref, back_x_ref, back_z_ref, mine_ref, out_ref, sums_ref, wide_ref, *, size, owners):
    per, own = size // (2 * owners), size // owners
    group = per * own
    wide = dot(halves(field_ref[...]), z_ref[...])
    for part in range(2):
        wide_ref[part] = wide[:, part * size : (part + 1) * size]

    def planes(y, part):
        return [wide_ref[part, pl.ds(y * per + t, owners, stride=group), :] for t in range(per)]

    columns = [jnp.concatenate(planes(y, 0) + planes(y, 1), axis=0) for y in range(own)]
    wave = dot(x_ref[...], halves(jnp.concatenate(columns, axis=1)))
    scale = jnp.concatenate([potential_ref[:, y, :] for y in range(own)], axis=1)
    product = jnp.concatenate([wave[:size] * scale, wave[size:] * scale], axis=0)
    back = dot(back_x_ref[...], halves(product))
    for y in range(own):
        for t in range(per):
            for part in range(2):
                first = (part * per + t) * owners
                wide_ref[part, pl.ds(y * per + t, owners, stride=group), :] = back[first : first + owners, y * size : (y + 1) * size]
    product = dot(halves(jnp.concatenate([wide_ref[0], wide_ref[1]], axis=1)), back_z_ref[...])
    out_ref[...] = product
    sums_ref[...] = overlaps(mine_ref, product, owners)


def overlaps(fields_ref, product, owners):
    half = product.shape[1] // 2
    crossed = jnp.concatenate([product[:, half:], -product[:, :half]], axis=1)
    fields = [fields_ref[m, :owners].reshape(product.shape) for m in range(fields_ref.shape[0])]
    return jnp.concatenate([jnp.sum(f * other, axis=0, keepdims=True) for other in (product, crossed) for f in fields], axis=0)


def pair_kernel(theirs_ref, product_ref, sums_ref, out_ref, *, owners):
    lanes = product_ref.shape[1]
    group = product_ref.shape[0] // owners
    sums = jnp.concatenate([sums_ref[...], overlaps(theirs_ref, product_ref[...], owners)], axis=0)
    sums = jnp.dot(sums, jnp.ones((lanes, lanes), jnp.float32), precision=highest, preferred_element_type=jnp.float32)
    on_diagonal = lax.broadcasted_iota(jnp.int32, sums.shape, 0) == lax.broadcasted_iota(jnp.int32, sums.shape, 1)
    row = jnp.sum(jnp.where(on_diagonal, sums, 0.0), axis=0, keepdims=True)
    for r in range(group):
        out_ref[pl.ds(r, owners, stride=group + 1), :] = product_ref[pl.ds(r, owners, stride=group), :]
    out_ref[pl.ds(group, owners, stride=group + 1), :] = jnp.broadcast_to(row, (owners, lanes))


def project_kernel(core_ref, occupied_ref, rows_ref, at_ref, along_ref, mine_ref, theirs_ref, out_ref, *, size, owners, coefs):
    chips = mine_ref.shape[0]
    bands = 2 * chips
    half = size // 2
    group = rows_ref.shape[0] // owners
    planes = half // owners
    sums = jnp.sum(rows_ref[pl.ds(group - 1, owners, stride=group), :], axis=0, keepdims=True)
    fields = []
    for t in range(planes):
        rows = [rows_ref[pl.ds(r, owners, stride=group), :] for r in range(t, group - 1, planes)]
        fields.append(jnp.concatenate(rows, axis=0))
    both = dot(along_ref[...], halves(jnp.concatenate(fields, axis=1)))
    by_cosine, by_sine = (
        jnp.concatenate([x[:, t * size : (t + 1) * size] for t in range(planes)], axis=0).T for x in (both[:half], both[half:])
    )
    lines = jnp.concatenate([by_cosine[:half] + by_sine[half:], by_cosine[half:] - by_sine[:half]], axis=0)
    lines = jnp.concatenate(halves(lines), axis=1)
    tall, lanes = out_ref.shape[1:]
    taken = [jnp.zeros((tall, lanes), jnp.float32) for _ in range(2)]
    core = core_ref[0]
    for m in range(bands):
        held, first, source, from_core = (mine_ref, 0, m, core) if m < chips else (theirs_ref, 2 * chips, m - chips, 1 - core)
        share = occupied_ref[2 * row(chips)[source] + from_core].astype(jnp.float32) * (1.0 / coefs)
        weight_real = sums[:, first + source : first + source + 1] * share
        weight_imag = sums[:, first + chips + source : first + chips + source + 1] * share
        basis = held[source, owners:].reshape(2, tall, lanes)
        taken[0] = taken[0] + weight_real * basis[0] - weight_imag * basis[1]
        taken[1] = taken[1] + weight_imag * basis[0] + weight_real * basis[1]
    every_line = numbered(planes * half, lanes)
    every_column = lax.broadcasted_iota(jnp.int32, (half, lanes), 0).astype(jnp.float32)
    one, zero = jnp.ones((), jnp.bfloat16), jnp.zeros((), jnp.bfloat16)
    for r in range(0, tall, 2):
        at_line = [jnp.where(every_line == copied_down(at_ref[0, i : i + 1, :], planes * half), one, zero) for i in (r, r + 1)]
        at_line = jnp.concatenate(at_line, axis=1)
        found = jnp.dot(lines, jnp.concatenate([at_line, at_line], axis=0), preferred_element_type=jnp.float32)
        for i in range(2):
            at_column = every_column == at_ref[1, r + i : r + i + 1, :]
            for p in range(2):
                applied = jnp.where(at_column, found[p * half : (p + 1) * half, i * lanes : (i + 1) * lanes], 0.0)
                out_ref[p, r + i : r + i + 1, :] = jnp.sum(applied, axis=0, keepdims=True) - taken[p][r + i : r + i + 1]


SCALARS = pl.BlockSpec(memory_space=pltpu.SMEM)
FAR = pl.BlockSpec(memory_space=pl.ANY)
WHOLE = pl.BlockSpec(memory_space=pltpu.VMEM)


def spread(owner, core, psi, points, table, size, owners):
    return pl.pallas_call(
        functools.partial(spread_kernel, size=size, owners=owners),
        out_shape=(made((size * (size // (2 * owners)), size)), made((2, *points.shape[1:]))),
        in_specs=[SCALARS, SCALARS, FAR, FAR, FAR],
        scratch_shapes=[
            pltpu.VMEM(psi.shape, psi.dtype),
            pltpu.VMEM(points.shape[1:], points.dtype),
            pltpu.VMEM(table.shape, table.dtype),
            pltpu.VMEM((4, *points.shape[1:]), jnp.float32),
            pltpu.SemaphoreType.DMA((3,)),
        ],
        interpret=INTERPRET,
        name="spread",
    )(owner, core, psi, points, table)


def fan(rows, psi, copies):
    shape = (copies, rows.shape[0] + psi.shape[0], *rows.shape[1:])
    return pl.pallas_call(fan_kernel, out_shape=made(shape), interpret=INTERPRET, name="fan")(near(rows), near(psi))


def apply(field, potential, along_z, along_x, back_x, back_z, mine, size, owners):
    return pl.pallas_call(
        functools.partial(apply_kernel, size=size, owners=owners),
        out_shape=(made(field.shape), made((2 * mine.shape[0], size))),
        scratch_shapes=[pltpu.VMEM((2, *field.shape), jnp.float32)],
        interpret=INTERPRET,
        name="apply",
    )(*map(near, (field, potential, along_z, along_x, back_x, back_z, mine)))


def pair(theirs, product, sums, owners):
    return pl.pallas_call(
        functools.partial(pair_kernel, owners=owners),
        out_shape=made((product.shape[0] + owners, product.shape[1])),
        interpret=INTERPRET,
        name="pair",
    )(*map(near, (theirs, product, sums)))


def project(core, occupied, rows, at, table, mine, theirs, size, owners, coefs):
    return pl.pallas_call(
        functools.partial(project_kernel, size=size, owners=owners, coefs=coefs),
        out_shape=jax.ShapeDtypeStruct(at.shape, jnp.float32),
        in_specs=[SCALARS, SCALARS] + [WHOLE] * 5,
        interpret=INTERPRET,
        name="project",
    )(core, occupied, *map(near, (rows, at, table, mine, theirs)))


def exchanged(x, axis, order):
    return lax.all_to_all(x, axis, split_axis=0, concat_axis=0, axis_index_groups=[order], tiled=True)


def along_ring(x, axis, step):
    count = lax.axis_size(axis)
    return lax.ppermute(x, axis, [(i, (i + step) % count) for i in range(count)])


def shards(psi, potential, miller, occupied):
    size = potential.shape[0]
    owners, chips = lax.axis_size("ga"), lax.axis_size("chip")
    block = psi.shape[2]
    along_y, along_z, along_x, back_x, back_z, back_y = tables(size, owners)
    owner, core = (lax.axis_index(axis).reshape(1) for axis in ("ga", "core"))
    points = miller.reshape(-1, block // size, size)
    rows, at = spread(owner, core, psi.reshape(2, -1, size), points, along_y, size, owners)
    group = rows.shape[0] // owners
    rows = exchanged(rows.reshape(owners, group, size), "ga", ring(owners))
    sent = fan(rows, psi.reshape(-1, group, size), chips)
    mine = exchanged(sent, "chip", row(chips))
    theirs = along_ring(mine, "core", 1)
    product, sums = apply(rows.reshape(-1, size), potential, along_z, along_x, back_x, back_z, mine, size, owners)
    sent = pair(theirs, product, sums, owners)
    rows = exchanged(sent.reshape(owners, 1, -1), "ga", ring(owners)).reshape(sent.shape)
    out = project(core, occupied, rows, at, back_y, mine, theirs, size, owners, miller.shape[0])
    return out.reshape(2, 1, block)


def solution(mesh):
    groups, owners, bands = (mesh.shape[axis] for axis in ("pert", "ga", "band"))
    mesh = Mesh(mesh.devices.reshape(groups, owners, bands // 2, 2), ("pert", "ga", "chip", "core"))
    in_specs = (P(None, ("chip", "core"), "ga"), P("pert", "ga", None), P(), P())
    out_specs = P(None, ("pert", "chip", "core"), "ga")
    return jax.shard_map(shards, mesh=mesh, in_specs=in_specs, out_specs=out_specs, check_vma=False)
```

```python
import functools

import jax
import jax.numpy as jnp
import numpy as np
from jax import lax
from jax.experimental import pallas as pl
from jax.experimental.pallas import tpu as pltpu
from jax.sharding import Mesh
from jax.sharding import PartitionSpec as P

highest = lax.Precision.HIGHEST
INTERPRET = False


def near(x):
    return x if INTERPRET else pltpu.with_memory_space_constraint(x, pltpu.VMEM)


def made(shape, dtype=jnp.float32):
    return jax.ShapeDtypeStruct(shape, dtype) if INTERPRET else pltpu.VMEM(shape, dtype)


def halves(x):
    high = x.astype(jnp.bfloat16)
    return high, (x - high.astype(jnp.float32)).astype(jnp.bfloat16)


def dot(a, b):
    part = functools.partial(jnp.dot, preferred_element_type=jnp.float32)
    return part(a[0], b[0]) + (part(a[0], b[1]) + part(a[1], b[0]))


def turned(x):
    half = x.shape[1] // 2
    return jnp.concatenate([-x[:, half:], x[:, :half]], axis=1)


def listed(count, first):
    return [(first + i) % count for i in range(count)]


def ring(owners):
    return listed(owners, owners * 7 // 8)


def row(chips):
    return listed(chips, chips // 2)


def tables(size, owners):
    order = np.asarray(ring(owners))
    signed = np.arange(size // 2) - size // 4
    angle = 2.0 * np.pi / size * (np.arange(size)[:, None] * signed[None, :] % size)
    cosine, sine = np.cos(angle), np.sin(angle)
    by_owner = [part.reshape(owners, size // owners, -1)[order] for part in (cosine, sine)]
    along_y = np.concatenate([part.reshape(size, -1) for part in by_owner], axis=1)
    along_z = np.block([[cosine.T, sine.T], [-sine.T, cosine.T]])
    planes = [part.reshape(size, -1, owners)[:, :, order].reshape(size, -1) for part in (cosine, sine)]
    along_x = np.block([[planes[0], -planes[1]], [planes[1], planes[0]]])
    back = [part.transpose(2, 1, 0).reshape(size // 2, size) for part in by_owner]
    back_y = np.concatenate(back, axis=0)

    def both(table):
        table = np.asarray(table, np.float32)
        high = table.astype(jnp.bfloat16)
        return np.stack([high, (table - high.astype(np.float32)).astype(jnp.bfloat16)])

    return tuple(map(both, (along_y, along_z, along_x, along_x.T, along_z.T / size**3, back_y)))


def places(points, size, owners):
    quarter = size // 4
    plane = (points // (size * size) + quarter) % size
    row = (points // size + quarter) % size
    column = (points + quarter) % size
    return plane // owners * (size // 2) + row, column


def own_points(owner_ref, points_ref, held_ref, sem):
    return pltpu.make_async_copy(points_ref.at[owner_ref[0]], held_ref, sem)


def numbered(count, lanes):
    return lax.broadcasted_iota(jnp.int32, (count, lanes), 0).astype(jnp.float32).astype(jnp.bfloat16)


def copied_down(row, count):
    some = jnp.broadcast_to(row, (16, row.shape[1])).astype(jnp.bfloat16)
    return jnp.concatenate([some] * (count // 16), axis=0)


def spread_kernel(
    owner_ref, core_ref, psi_ref, points_ref, along_ref, out_ref, at_ref, psi_held, points_held, along_held, flat_ref, sems, *, size, owners
):
    del core_ref
    copies = [
        own_points(owner_ref, points_ref, points_held, sems.at[0]),
        pltpu.make_async_copy(psi_ref, psi_held, sems.at[1]),
        pltpu.make_async_copy(along_ref, along_held, sems.at[2]),
    ]
    for copy in copies:
        copy.start()
    half = size // 2
    lines = half * half // owners
    copies[0].wait()
    for i, x in enumerate(places(points_held[...], size, owners)):
        at_ref[i] = x.astype(jnp.float32)
    copies[1].wait()
    for part in range(2):
        for which, x in enumerate(halves(psi_held[part])):
            flat_ref[2 * which + part] = x.astype(jnp.float32)
    tall, lanes = points_held.shape
    every_line, every_column = numbered(lines, lanes), numbered(half, lanes)
    one, zero = jnp.ones((), jnp.bfloat16), jnp.zeros((), jnp.bfloat16)
    at_line, values = [], []
    for r in range(tall):
        at_line.append(jnp.where(every_line == copied_down(at_ref[0, r : r + 1, :], lines), one, zero))
        at_column = every_column == copied_down(at_ref[1, r : r + 1, :], half)
        parts = [jnp.where(at_column, copied_down(flat_ref[i, r : r + 1, :], half), zero) for i in range(4)]
        values.append(jnp.concatenate(parts, axis=0))
    at_line, values = jnp.concatenate(at_line, axis=1), jnp.concatenate(values, axis=1)
    total = lax.dot_general(at_line, values, (((1,), (1,)), ((), ())), preferred_element_type=jnp.float32)
    total = total[:, :size] + total[:, size:]
    around = turned(total)
    planes = lines // half
    fields = [jnp.concatenate([x[t * half : (t + 1) * half] for x in (total, around)], axis=0) for t in range(planes)]
    copies[2].wait()
    rows = dot(along_held[...], halves(jnp.concatenate(fields, axis=1)))
    for t in range(planes):
        out_ref[pl.ds(t, size, stride=planes), :] = rows[:, t * size : (t + 1) * size]


def fan_kernel(rows_ref, psi_ref, out_ref):
    for i in range(out_ref.shape[0]):
        out_ref[i, : rows_ref.shape[0]] = rows_ref[...]
        out_ref[i, rows_ref.shape[0] :] = psi_ref[...]


def apply_kernel(field_ref, potential_ref, z_ref, x_ref, back_x_ref, back_z_ref, mine_ref, out_ref, sums_ref, wide_ref, *, size, owners):
    per, own = size // (2 * owners), size // owners
    group = per * own
    wide = dot(halves(field_ref[...]), z_ref[...])
    for part in range(2):
        wide_ref[part] = wide[:, part * size : (part + 1) * size]

    def planes(y, part):
        return [wide_ref[part, pl.ds(y * per + t, owners, stride=group), :] for t in range(per)]

    columns = [jnp.concatenate(planes(y, 0) + planes(y, 1), axis=0) for y in range(own)]
    wave = dot(x_ref[...], halves(jnp.concatenate(columns, axis=1)))
    scale = jnp.concatenate([potential_ref[:, y, :] for y in range(own)], axis=1)
    product = jnp.concatenate([wave[:size] * scale, wave[size:] * scale], axis=0)
    back = dot(back_x_ref[...], halves(product))
    for y in range(own):
        for t in range(per):
            for part in range(2):
                first = (part * per + t) * owners
                wide_ref[part, pl.ds(y * per + t, owners, stride=group), :] = back[first : first + owners, y * size : (y + 1) * size]
    product = dot(halves(jnp.concatenate([wide_ref[0], wide_ref[1]], axis=1)), back_z_ref[...])
    out_ref[...] = product
    sums_ref[...] = overlaps(mine_ref, product, owners)


def overlaps(fields_ref, product, owners):
    half = product.shape[1] // 2
    crossed = jnp.concatenate([product[:, half:], -product[:, :half]], axis=1)
    fields = [fields_ref[m, :owners].reshape(product.shape) for m in range(fields_ref.shape[0])]
    return jnp.concatenate([jnp.sum(f * other, axis=0, keepdims=True) for other in (product, crossed) for f in fields], axis=0)


def pair_kernel(theirs_ref, product_ref, sums_ref, out_ref, *, owners):
    lanes = product_ref.shape[1]
    group = product_ref.shape[0] // owners
    sums = jnp.concatenate([sums_ref[...], overlaps(theirs_ref, product_ref[...], owners)], axis=0)
    sums = jnp.dot(sums, jnp.ones((lanes, lanes), jnp.float32), precision=highest, preferred_element_type=jnp.float32)
    on_diagonal = lax.broadcasted_iota(jnp.int32, sums.shape, 0) == lax.broadcasted_iota(jnp.int32, sums.shape, 1)
    row = jnp.sum(jnp.where(on_diagonal, sums, 0.0), axis=0, keepdims=True)
    for r in range(group):
        out_ref[pl.ds(r, owners, stride=group + 1), :] = product_ref[pl.ds(r, owners, stride=group), :]
    out_ref[pl.ds(group, owners, stride=group + 1), :] = jnp.broadcast_to(row, (owners, lanes))


def project_kernel(core_ref, occupied_ref, rows_ref, at_ref, along_ref, mine_ref, theirs_ref, out_ref, *, size, owners, coefs):
    chips = mine_ref.shape[0]
    bands = 2 * chips
    half = size // 2
    group = rows_ref.shape[0] // owners
    planes = half // owners
    sums = jnp.sum(rows_ref[pl.ds(group - 1, owners, stride=group), :], axis=0, keepdims=True)
    fields = []
    for t in range(planes):
        rows = [rows_ref[pl.ds(r, owners, stride=group), :] for r in range(t, group - 1, planes)]
        fields.append(jnp.concatenate(rows, axis=0))
    both = dot(along_ref[...], halves(jnp.concatenate(fields, axis=1)))
    by_cosine, by_sine = (
        jnp.concatenate([x[:, t * size : (t + 1) * size] for t in range(planes)], axis=0).T for x in (both[:half], both[half:])
    )
    lines = jnp.concatenate([by_cosine[:half] + by_sine[half:], by_cosine[half:] - by_sine[:half]], axis=0)
    lines = jnp.concatenate(halves(lines), axis=1)
    tall, lanes = out_ref.shape[1:]
    taken = [jnp.zeros((tall, lanes), jnp.float32) for _ in range(2)]
    core = core_ref[0]
    for m in range(bands):
        held, first, source, from_core = (mine_ref, 0, m, core) if m < chips else (theirs_ref, 2 * chips, m - chips, 1 - core)
        share = occupied_ref[2 * row(chips)[source] + from_core].astype(jnp.float32) * (1.0 / coefs)
        weight_real = sums[:, first + source : first + source + 1] * share
        weight_imag = sums[:, first + chips + source : first + chips + source + 1] * share
        basis = held[source, owners:].reshape(2, tall, lanes)
        taken[0] = taken[0] + weight_real * basis[0] - weight_imag * basis[1]
        taken[1] = taken[1] + weight_imag * basis[0] + weight_real * basis[1]
    every_line = numbered(planes * half, lanes)
    every_column = lax.broadcasted_iota(jnp.int32, (half, lanes), 0).astype(jnp.float32)
    one, zero = jnp.ones((), jnp.bfloat16), jnp.zeros((), jnp.bfloat16)
    for r in range(0, tall, 2):
        at_line = [jnp.where(every_line == copied_down(at_ref[0, i : i + 1, :], planes * half), one, zero) for i in (r, r + 1)]
        at_line = jnp.concatenate(at_line, axis=1)
        found = jnp.dot(lines, jnp.concatenate([at_line, at_line], axis=0), preferred_element_type=jnp.float32)
        for i in range(2):
            at_column = every_column == at_ref[1, r + i : r + i + 1, :]
            for p in range(2):
                applied = jnp.where(at_column, found[p * half : (p + 1) * half, i * lanes : (i + 1) * lanes], 0.0)
                out_ref[p, r + i : r + i + 1, :] = jnp.sum(applied, axis=0, keepdims=True) - taken[p][r + i : r + i + 1]


SCALARS = pl.BlockSpec(memory_space=pltpu.SMEM)
FAR = pl.BlockSpec(memory_space=pl.ANY)
WHOLE = pl.BlockSpec(memory_space=pltpu.VMEM)


def spread(owner, core, psi, points, table, size, owners):
    return pl.pallas_call(
        functools.partial(spread_kernel, size=size, owners=owners),
        out_shape=(made((size * (size // (2 * owners)), size)), made((2, *points.shape[1:]))),
        in_specs=[SCALARS, SCALARS, FAR, FAR, FAR],
        scratch_shapes=[
            pltpu.VMEM(psi.shape, psi.dtype),
            pltpu.VMEM(points.shape[1:], points.dtype),
            pltpu.VMEM(table.shape, table.dtype),
            pltpu.VMEM((4, *points.shape[1:]), jnp.float32),
            pltpu.SemaphoreType.DMA((3,)),
        ],
        interpret=INTERPRET,
        name="spread",
    )(owner, core, psi, points, table)


def fan(rows, psi, copies):
    shape = (copies, rows.shape[0] + psi.shape[0], *rows.shape[1:])
    return pl.pallas_call(fan_kernel, out_shape=made(shape), interpret=INTERPRET, name="fan")(near(rows), near(psi))


def apply(field, potential, along_z, along_x, back_x, back_z, mine, size, owners):
    return pl.pallas_call(
        functools.partial(apply_kernel, size=size, owners=owners),
        out_shape=(made(field.shape), made((2 * mine.shape[0], size))),
        scratch_shapes=[pltpu.VMEM((2, *field.shape), jnp.float32)],
        interpret=INTERPRET,
        name="apply",
    )(*map(near, (field, potential, along_z, along_x, back_x, back_z, mine)))


def pair(theirs, product, sums, owners):
    return pl.pallas_call(
        functools.partial(pair_kernel, owners=owners),
        out_shape=made((product.shape[0] + owners, product.shape[1])),
        interpret=INTERPRET,
        name="pair",
    )(*map(near, (theirs, product, sums)))


def project(core, occupied, rows, at, table, mine, theirs, size, owners, coefs):
    return pl.pallas_call(
        functools.partial(project_kernel, size=size, owners=owners, coefs=coefs),
        out_shape=jax.ShapeDtypeStruct(at.shape, jnp.float32),
        in_specs=[SCALARS, SCALARS] + [WHOLE] * 5,
        interpret=INTERPRET,
        name="project",
    )(core, occupied, *map(near, (rows, at, table, mine, theirs)))


def exchanged(x, axis, order):
    return lax.all_to_all(x, axis, split_axis=0, concat_axis=0, axis_index_groups=[order], tiled=True)


def along_ring(x, axis, step):
    count = lax.axis_size(axis)
    return lax.ppermute(x, axis, [(i, (i + step) % count) for i in range(count)])


def shards(psi, potential, miller, occupied):
    size = potential.shape[0]
    owners, chips = lax.axis_size("ga"), lax.axis_size("chip")
    block = psi.shape[2]
    along_y, along_z, along_x, back_x, back_z, back_y = tables(size, owners)
    owner, core = (lax.axis_index(axis).reshape(1) for axis in ("ga", "core"))
    points = miller.reshape(-1, block // size, size)
    rows, at = spread(owner, core, psi.reshape(2, -1, size), points, along_y, size, owners)
    group = rows.shape[0] // owners
    rows = exchanged(rows.reshape(owners, group, size), "ga", ring(owners))
    sent = fan(rows, psi.reshape(-1, group, size), chips)
    mine = exchanged(sent, "chip", row(chips))
    theirs = along_ring(mine, "core", 1)
    product, sums = apply(rows.reshape(-1, size), potential, along_z, along_x, back_x, back_z, mine, size, owners)
    sent = pair(theirs, product, sums, owners)
    rows = exchanged(sent.reshape(owners, 1, -1), "ga", ring(owners)).reshape(sent.shape)
    out = project(core, occupied, rows, at, back_y, mine, theirs, size, owners, miller.shape[0])
    return out.reshape(2, 1, block)


def solution(mesh):
    groups, owners, bands = (mesh.shape[axis] for axis in ("pert", "ga", "band"))
    mesh = Mesh(mesh.devices.reshape(groups, owners, bands // 2, 2), ("pert", "ga", "chip", "core"))
    in_specs = (P(None, ("chip", "core"), "ga"), P("pert", "ga", None), P(), P())
    out_specs = P(None, ("pert", "chip", "core"), "ga")
    return jax.shard_map(shards, mesh=mesh, in_specs=in_specs, out_specs=out_specs, check_vma=False)
```
